256 devices in a mesh: freq: 16 (over z, core), tm: 16 (over y, x).
Axes of the slice: x: 4, y: 4, z: 8, core: 2. Of those that a mesh axis runs over, the one named last changes fastest.
Arguments:
- band_state: float32 [2048, 16384], P('freq', 'tm'), may hold values from -2.5 to 2.5
- lower_rows: int32 [3, 2048], replicated, may hold values from 0 to 2047, as said below
- upper_rows: int32 [3, 2048], replicated, may hold values from 0 to 2047, as said below
- delays: int32 [3, 2048], replicated, may hold values from 0 to 1024, as said below
- counts: int32 [7], replicated, may hold values from 256 to 2048, as said below
Outputs:
- dedispersed: float32 [2048, 16384], P('freq', 'tm')
The draws below stay inside these ranges and needn't reach their ends.
Inputs may be any that keep to these rules, and one draw needn't show every extreme that they name: `counts`: entry 8 - 8 / 2^k + b is the live row count of output sub-band b of iteration k; it lies between half and all of that sub-band's 2 * 2048 / 2^(3 - k) padded rows, and in every iteration some sub-band has all its rows live. With w = 2048 / 2^(3 - k), lower_rows[k, i] is a row of input sub-band 2 * floor(i / (2 * w)) whose position in that sub-band is below its live count (all w rows are live in iteration 0). With w = 2048 / 2^(3 - k), upper_rows[k, i] is a row of input sub-band 2 * floor(i / (2 * w)) + 1 whose position in that sub-band is below its live count (all w rows are live in iteration 0). delays[k, i] is at most 2048 / 2^(3 - k), and equals it at some row in every iteration.
All inputs are finite; a program needn't handle non-finite values.
Results may differ from the reference program's by a relative error of at most 0.0003.
Values sent between devices are 32-bit elements; how exact they have to be, the bound alone decides.
A program may use at most 64 MiB of HBM per device.

```python
import jax
import jax.numpy as jnp
from jax import lax

DMAX = 2048
ITERS = 3
NT = 16384


def table_draws(key):
    count_parts = []
    lower_parts = []
    upper_parts = []
    delay_parts = []
    all_rows = jnp.arange(DMAX, dtype=jnp.int32)
    previous = jnp.full((2 ** ITERS,), DMAX >> ITERS, jnp.int32)
    for iteration in range(ITERS):
        width_in = DMAX >> ITERS - iteration
        width_out = 2 * width_in
        bands_out = DMAX // width_out
        level_keys = jax.random.split(jax.random.fold_in(key, 101 + iteration), 6)
        fresh_counts = jax.random.randint(level_keys[0], (bands_out,), width_out // 2, width_out + 1, dtype=jnp.int32)
        full_band = jax.random.randint(level_keys[5], (), 0, bands_out, dtype=jnp.int32)
        fresh_counts = jnp.where(jnp.arange(bands_out, dtype=jnp.int32) == full_band, width_out, fresh_counts)
        band_index = all_rows // width_out
        lower_live = previous[2 * band_index]
        upper_live = previous[2 * band_index + 1]
        lower_pick = jax.random.randint(level_keys[1], (DMAX,), 0, 1 << 30, dtype=jnp.int32) % lower_live
        upper_pick = jax.random.randint(level_keys[2], (DMAX,), 0, 1 << 30, dtype=jnp.int32) % upper_live
        delay_pick = jax.random.randint(level_keys[3], (DMAX,), 0, width_in + 1, dtype=jnp.int32)
        spot_row = jax.random.randint(level_keys[4], (), 0, DMAX, dtype=jnp.int32)
        delay_pick = jnp.where(all_rows == spot_row, width_in, delay_pick)
        count_parts.append(fresh_counts)
        lower_parts.append(2 * band_index * width_in + lower_pick)
        upper_parts.append((2 * band_index + 1) * width_in + upper_pick)
        delay_parts.append(delay_pick)
        previous = fresh_counts
    return (jnp.concatenate(count_parts), jnp.stack(lower_parts), jnp.stack(upper_parts), jnp.stack(delay_parts))


def draw_counts(key, part):
    return table_draws(key)[0]


def draw_lower_rows(key, part):
    return table_draws(key)[1]


def draw_upper_rows(key, part):
    return table_draws(key)[2]


def draw_delays(key, part):
    return table_draws(key)[3]


def block_levels(stream_key, dims, shards, smallest, top_value):
    def one(position, parts):
        draws = jax.random.uniform(jax.random.fold_in(jax.random.fold_in(stream_key, 6), position), (parts,), jnp.float32, smallest / len(shards), top_value / len(shards))
        return jnp.repeat(jnp.exp(draws), dims[position] // parts).reshape((-1,) + (1,) * (len(dims) - position - 1))

    loudness = one(*shards[0])
    for cut in shards[1:]:
        loudness = loudness * one(*cut)
    return loudness


def noise(key, dims, spread, limit, cuts=(), held_as=jnp.bfloat16):
    drawn = spread * jax.random.normal(key, dims, jnp.float32)
    if cuts:
        drawn = drawn * block_levels(key, dims, cuts, -0.22, 0.18)
    return jnp.clip(drawn, -limit, limit).astype(held_as)


def setup_inputs(seed: int = 0) -> dict:
    streams_of = jax.random.split(jax.random.key(seed), 6)
    band_state = noise(streams_of[0], (DMAX, NT), 0.35, 2.5, ((0, 16), (1, 16)), jnp.float32)
    lower_rows = draw_lower_rows(jax.random.fold_in(streams_of[5], 71), 0)
    upper_rows = draw_upper_rows(jax.random.fold_in(streams_of[5], 71), 0)
    delays = draw_delays(jax.random.fold_in(streams_of[5], 71), 0)
    counts = draw_counts(jax.random.fold_in(streams_of[5], 71), 0)
    return {"band_state": band_state, "lower_rows": lower_rows, "upper_rows": upper_rows, "delays": delays, "counts": counts}


def delayed_rows(source_rows, shifts):
    positions = jnp.arange(source_rows.shape[1], dtype=jnp.int32)[None, :] - shifts[:, None]
    picked = jnp.take_along_axis(source_rows, jnp.maximum(positions, 0), axis=1)
    return jnp.where(positions >= 0, picked, jnp.zeros_like(picked))


def reference(band_state, lower_rows, upper_rows, delays, counts):
    block_rows = min(DMAX, 512)
    all_rows = jnp.arange(DMAX, dtype=jnp.int32)
    current = band_state
    for iteration in range(ITERS):
        width_out = DMAX >> (ITERS - iteration - 1)
        offset = 2 ** ITERS - 2 ** (ITERS - iteration)
        live_rows = (all_rows % width_out) < counts[offset + all_rows // width_out]

        def merge_block(pieces, current=current):
            lower_index, upper_index, shifts, keep_rows = pieces
            summed = current[lower_index] + delayed_rows(current[upper_index], shifts)
            return jnp.where(keep_rows[:, None], summed, jnp.zeros_like(summed))

        pieces = (lower_rows[iteration].reshape(-1, block_rows),
                  upper_rows[iteration].reshape(-1, block_rows),
                  delays[iteration].reshape(-1, block_rows),
                  live_rows.reshape(-1, block_rows))
        merged = lax.map(merge_block, pieces)
        current = merged.reshape(DMAX, -1)
    return current
```

```python
import jax
import jax.numpy as jnp
from jax import lax
from jax.experimental import pallas as pl
from jax.experimental.pallas import tpu as pltpu
from jax.sharding import PartitionSpec as P

DMAX = 2048
ITERS = 3
MESH = pl.DeviceIdType.MESH

CHIPS = 8
ROWS = 128
GROUPS = 32
TILES = 23
SPAN = TILES * 8
PAD, FAR, NEAR, OWN = 0, 1, 7, 15
UNIT = 32
HALF_UNITS = 64 // UNIT
ZERO_ROW = GROUPS * SPAN


def kernel(
    x, lower, upper, delays, counts, out,
    raw, select, delay, live, picks, sent, landed, result,
    local_sem, table_sem, near_sem, far_sem, own_sem, history_sem, send_sem, recv_sem, out_sem,
):
    freq = lax.axis_index("freq")
    tm = lax.axis_index("tm")
    tm_count = lax.axis_size("tm")
    z = lax.div(freq, 2)
    core = lax.rem(freq, 2)
    bits = [lax.rem(z, 2), lax.rem(lax.div(z, 2), 2), lax.div(z, 4)]
    partner = freq + 1 - 2 * core
    freq_up = lax.rem(freq + 2, 16)
    freq_down = lax.rem(freq + 14, 16)
    ring = (freq_up, freq_down)
    flat = raw.reshape((GROUPS + 1) * SPAN, 128)
    mine = pl.ds(core * 16, 16)
    theirs = pl.ds(16 - core * 16, 16)

    own = pltpu.make_async_copy(x, raw.at[mine, pl.ds(OWN * 8, 64), :], local_sem)
    own.start()
    tables = [
        pltpu.make_async_copy(source, target, table_sem.at[n])
        for n, (source, target) in enumerate(
            ((lower, select.at[0]), (upper, select.at[1]), (delays, delay), (counts, live))
        )
    ]
    for table in tables:
        table.start()

    barrier = pltpu.get_barrier_semaphore()
    peers = [
        {"freq": partner}, {"freq": freq_up}, {"freq": freq_down},
        {"tm": lax.rem(tm + 1, tm_count)}, {"tm": lax.rem(tm + tm_count - 1, tm_count)},
        {"tm": lax.rem(tm + 2, tm_count)}, {"tm": lax.rem(tm + tm_count - 2, tm_count)},
    ]
    for peer in peers:
        pl.semaphore_signal(barrier, inc=1, device_id=peer, device_id_type=MESH)
    pl.semaphore_wait(barrier, len(peers))

    own.wait()

    def remote(source, target, send, recv, device):
        return pltpu.make_async_remote_copy(
            src_ref=source, dst_ref=target, send_sem=send, recv_sem=recv,
            device_id=device, device_id_type=MESH,
        )

    near = remote(
        raw.at[mine, pl.ds(OWN * 8, 64), :], raw.at[mine, pl.ds(NEAR * 8, 64), :],
        near_sem.at[0], near_sem.at[1], {"tm": lax.rem(tm + 1, tm_count)},
    )
    far = remote(
        raw.at[mine, pl.ds((OWN + 2) * 8, 48), :], raw.at[mine, pl.ds(FAR * 8, 48), :],
        far_sem.at[0], far_sem.at[1], {"tm": lax.rem(tm + 2, tm_count)},
    )
    to_partner = remote(
        raw.at[mine, pl.ds(OWN * 8, 64), :], raw.at[mine, pl.ds(OWN * 8, 64), :],
        own_sem.at[0], own_sem.at[1], {"freq": partner},
    )
    near_across = remote(
        raw.at[mine, pl.ds(NEAR * 8, 64), :], raw.at[mine, pl.ds(NEAR * 8, 64), :],
        history_sem.at[0], history_sem.at[1], {"freq": partner},
    )
    far_across = remote(
        raw.at[mine, pl.ds(FAR * 8, 48), :], raw.at[mine, pl.ds(FAR * 8, 48), :],
        history_sem.at[2], history_sem.at[3], {"freq": partner},
    )

    @pl.when(tm < tm_count - 1)
    def _():
        near.start()

    @pl.when(tm < tm_count - 2)
    def _():
        far.start()

    to_partner.start()

    def clear(first, count):
        def body(g, carry):
            raw[g, pl.ds(first * 8, count * 8), :] = jnp.zeros((count * 8, 128), jnp.float32)
            return carry
        lax.fori_loop(0, GROUPS, body, 0)

    raw[GROUPS, :, :] = jnp.zeros((SPAN, 128), jnp.float32)

    @pl.when(tm == 0)
    def _():
        clear(NEAR, 8)

    @pl.when(tm <= 1)
    def _():
        clear(FAR, 6)

    for table in tables:
        table.wait()

    def pick(row, slot):
        late = delay[2, row] * bits[2]
        top = select[bits[2], 2, row]
        late += delay[1, top] * bits[1]
        middle = select[bits[1], 1, top]
        late += delay[0, middle] * bits[0]
        bottom = select[bits[0], 0, middle] & 255
        alive = ((top & 1023) < live[4 + (top >> 10)]) & ((middle & 511) < live[middle >> 9])
        start = (bottom >> 3) * SPAN + (bottom & 7) + OWN * 8 - (late >> 7) * 8
        start = jnp.where(alive, start, ZERO_ROW + OWN * 8)
        picks[slot] = start * 128 + (late & 127)

    for offset in (4, 3, 5, 2, 6, 1, 7, 0):
        base = lax.rem(z + offset, CHIPS) * 256 + core * ROWS

        def body(step, carry, base=base, offset=offset):
            for k in range(8):
                pick(base + step * 8 + k, offset * ROWS + step * 8 + k)
            return carry

        lax.fori_loop(0, ROWS // 8, body, 0)

    @pl.when(tm > 0)
    def _():
        near.wait_recv()
        near_across.start()

    @pl.when(tm > 1)
    def _():
        far.wait_recv()
        far_across.start()

    to_partner.wait_recv()

    @pl.when(tm > 0)
    def _():
        near_across.wait_recv()

    @pl.when(tm > 1)
    def _():
        far_across.wait_recv()

    lanes = lax.broadcasted_iota(jnp.int32, (8, 128), 1)

    def contribution(slot):
        packed = picks[slot]
        start = packed >> 7
        shift = packed & 127
        same = flat[pl.ds(start, 8, stride=8), :]
        before = flat[pl.ds(start - 8, 8, stride=8), :]
        return pltpu.roll(jnp.where(lanes < 128 - shift, same, before), shift, 1)

    def message(direction, step, half, unit):
        return (direction * 4 + step) * 2 * HALF_UNITS + half * HALF_UNITS + unit

    def copy_of(direction, step, half, unit):
        index = message(direction, step, half, unit)
        return remote(
            sent.at[index], landed.at[index], send_sem.at[index], recv_sem.at[index],
            {"freq": ring[direction]},
        )

    def add_and_send(direction, step, half, unit):
        index = message(direction, step, half, unit)
        offset = 4 - step if direction == 0 else 4 + step
        first_slot = offset * ROWS + half * 64 + unit * UNIT
        fresh = step == 0 or (step == 1 and half != direction)
        if not fresh:
            copy_of(direction, step - 1, half, unit).wait_recv()
        previous = message(direction, step - 1, half, unit)

        def body(i, carry):
            for k in range(8):
                row = i * 8 + k
                value = contribution(first_slot + row)
                at = pl.ds(pl.multiple_of(row * 8, 8), 8)
                if not fresh:
                    value = value + landed[previous, at, :]
                sent[index, at, :] = value
            return carry

        lax.fori_loop(0, UNIT // 8, body, 0)
        copy_of(direction, step, half, unit).start()

    messages = []
    for step in range(4):
        for turn in range(2):
            if step == 0 and turn == 0:
                continue
            for unit in range(HALF_UNITS):
                for direction in range(2):
                    half = direction if turn == 1 else 1 - direction
                    messages.append((direction, step, half, unit))
    for entry in messages:
        add_and_send(*entry)

    first_row = freq * ROWS
    finished = []
    for half in range(2):
        for unit in range(HALF_UNITS):
            incoming = []
            for direction in range(2):
                copy_of(direction, 3, half, unit).wait_recv()
                incoming.append(message(direction, 3, half, unit))

            def body(i, carry, half=half, unit=unit, incoming=incoming):
                for k in range(8):
                    row = i * 8 + k
                    local = half * 64 + unit * UNIT + row
                    at = pl.ds(pl.multiple_of(row * 8, 8), 8)
                    value = contribution(local) + landed[incoming[0], at, :] + landed[incoming[1], at, :]
                    alive = first_row + local < live[6]
                    value = jnp.where(alive, value, jnp.zeros_like(value))
                    place = (half * 64 + unit * UNIT) * 8 + i * 64 + k
                    result[pl.ds(place, 8, stride=8), :] = value
                return carry

            lax.fori_loop(0, UNIT // 8, body, 0)
            index = half * HALF_UNITS + unit
            rows = pl.ds(index * UNIT * 8, UNIT * 8)
            write = pltpu.make_async_copy(result.at[rows, :], out.at[rows, :], out_sem.at[index])
            write.start()
            finished.append(write)

    @pl.when(tm < tm_count - 1)
    def _():
        near.wait_send()

    @pl.when(tm < tm_count - 2)
    def _():
        far.wait_send()

    to_partner.wait_send()

    @pl.when(tm > 0)
    def _():
        near_across.wait_send()

    @pl.when(tm > 1)
    def _():
        far_across.wait_send()

    for entry in messages:
        copy_of(*entry).wait_send()
    for write in finished:
        write.wait()


def per_device(band_state, lower_rows, upper_rows, delays, counts):
    tiles = band_state.reshape(16, 8, 8, 128).transpose(0, 2, 1, 3).reshape(16, 64, 128)
    message_count = 2 * 4 * 2 * HALF_UNITS
    dma = pltpu.SemaphoreType.DMA
    out = pl.pallas_call(
        kernel,
        out_shape=jax.ShapeDtypeStruct((1024, 128), jnp.float32),
        in_specs=[pl.BlockSpec(memory_space=pl.ANY)] * 5,
        out_specs=pl.BlockSpec(memory_space=pl.ANY),
        scratch_shapes=[
            pltpu.VMEM((GROUPS + 1, SPAN, 128), jnp.float32),
            pltpu.SMEM((2, ITERS, DMAX), jnp.int32),
            pltpu.SMEM((ITERS, DMAX), jnp.int32),
            pltpu.SMEM((7,), jnp.int32),
            pltpu.SMEM((CHIPS * ROWS,), jnp.int32),
            pltpu.VMEM((message_count, UNIT * 8, 128), jnp.float32),
            pltpu.VMEM((message_count, UNIT * 8, 128), jnp.float32),
            pltpu.VMEM((1024, 128), jnp.float32),
            dma,
            dma((4,)),
            dma((2,)),
            dma((2,)),
            dma((2,)),
            dma((4,)),
            dma((message_count,)),
            dma((message_count,)),
            dma((2 * HALF_UNITS,)),
        ],
        compiler_params=pltpu.CompilerParams(collective_id=0, has_side_effects=True, vmem_limit_bytes=40 << 20),
    )(tiles, lower_rows, upper_rows, delays, counts)
    return out.reshape(16, 8, 8, 128).transpose(0, 2, 1, 3).reshape(ROWS, 1024)


def solution(mesh):
    return jax.shard_map(
        per_device,
        mesh=mesh,
        in_specs=(P("freq", "tm"), P(), P(), P(), P()),
        out_specs=P("freq", "tm"),
        check_vma=False,
    )
```

```python
import jax
import jax.numpy as jnp
from jax import lax
from jax.experimental import pallas as pl
from jax.experimental.pallas import tpu as pltpu
from jax.sharding import PartitionSpec as P

DMAX = 2048
ITERS = 3
MESH = pl.DeviceIdType.MESH

CHIPS = 8
ROWS = 128
GROUPS = 32
TILES = 23
SPAN = TILES * 8
PAD, FAR, NEAR, OWN = 0, 1, 7, 15
UNIT = 32
HALF_UNITS = 64 // UNIT
ZERO_ROW = GROUPS * SPAN


def kernel(
    x, lower, upper, delays, counts, out,
    raw, lower_table, upper_table, delay_table, live, packed, picks, sent, landed,
    local_sem, table_sem, near_sem, far_sem, own_sem, history_sem, send_sem, recv_sem,
):
    freq = lax.axis_index("freq")
    tm = lax.axis_index("tm")
    tm_count = lax.axis_size("tm")
    z = lax.div(freq, 2)
    core = lax.rem(freq, 2)
    bits = [lax.rem(z, 2), lax.rem(lax.div(z, 2), 2), lax.div(z, 4)]
    partner = freq + 1 - 2 * core
    freq_up = lax.rem(freq + 2, 16)
    freq_down = lax.rem(freq + 14, 16)
    ring = (freq_up, freq_down)
    flat = raw.reshape((GROUPS + 1) * SPAN, 128)
    mine = pl.ds(core * 16, 16)
    theirs = pl.ds(16 - core * 16, 16)

    own = pltpu.make_async_copy(x, raw.at[mine, pl.ds(OWN * 8, 64), :], local_sem)
    own.start()
    tables = [
        pltpu.make_async_copy(source, target, table_sem.at[n])
        for n, (source, target) in enumerate(
            ((lower, lower_table), (upper, upper_table), (delays, delay_table), (counts, live))
        )
    ]
    for table in tables:
        table.start()

    barrier = pltpu.get_barrier_semaphore()
    peers = [
        {"freq": partner}, {"freq": freq_up}, {"freq": freq_down},
        {"tm": lax.rem(tm + 1, tm_count)}, {"tm": lax.rem(tm + tm_count - 1, tm_count)},
        {"tm": lax.rem(tm + 2, tm_count)}, {"tm": lax.rem(tm + tm_count - 2, tm_count)},
    ]
    for peer in peers:
        pl.semaphore_signal(barrier, inc=1, device_id=peer, device_id_type=MESH)
    pl.semaphore_wait(barrier, len(peers))

    own.wait()

    def remote(source, target, send, recv, device):
        return pltpu.make_async_remote_copy(
            src_ref=source, dst_ref=target, send_sem=send, recv_sem=recv,
            device_id=device, device_id_type=MESH,
        )

    near = remote(
        raw.at[mine, pl.ds(OWN * 8, 64), :], raw.at[mine, pl.ds(NEAR * 8, 64), :],
        near_sem.at[0], near_sem.at[1], {"tm": lax.rem(tm + 1, tm_count)},
    )
    far = remote(
        raw.at[mine, pl.ds((OWN + 2) * 8, 48), :], raw.at[mine, pl.ds(FAR * 8, 48), :],
        far_sem.at[0], far_sem.at[1], {"tm": lax.rem(tm + 2, tm_count)},
    )
    to_partner = remote(
        raw.at[mine, pl.ds(OWN * 8, 64), :], raw.at[mine, pl.ds(OWN * 8, 64), :],
        own_sem.at[0], own_sem.at[1], {"freq": partner},
    )
    near_across = remote(
        raw.at[mine, pl.ds(NEAR * 8, 64), :], raw.at[mine, pl.ds(NEAR * 8, 64), :],
        history_sem.at[0], history_sem.at[1], {"freq": partner},
    )
    far_across = remote(
        raw.at[mine, pl.ds(FAR * 8, 48), :], raw.at[mine, pl.ds(FAR * 8, 48), :],
        history_sem.at[2], history_sem.at[3], {"freq": partner},
    )

    @pl.when(tm < tm_count - 1)
    def _():
        near.start()

    @pl.when(tm < tm_count - 2)
    def _():
        far.start()

    to_partner.start()

    def clear(first, count):
        def body(g, carry):
            raw[g, pl.ds(first * 8, count * 8), :] = jnp.zeros((count * 8, 128), jnp.float32)
            return carry
        lax.fori_loop(0, GROUPS, body, 0)

    raw[GROUPS, :, :] = jnp.zeros((SPAN, 128), jnp.float32)

    @pl.when(tm == 0)
    def _():
        clear(NEAR, 8)

    @pl.when(tm <= 1)
    def _():
        clear(FAR, 6)

    for table in tables:
        table.wait()

    def entries(k, block):
        at = (pl.ds(k, 1), pl.ds(block, 128))
        row = jnp.where(bits[k] == 1, upper_table[at], lower_table[at])
        return row * 2048 + delay_table[at] * bits[k]

    def look_up(k, index):
        found = jnp.zeros((8, 128), jnp.int32)
        for block in range(DMAX // 128):
            table = jnp.broadcast_to(entries(k, block * 128), (8, 128))
            here = jnp.take_along_axis(table, index & 127, axis=1)
            found = jnp.where(index >> 7 == block, here, found)
        return found

    def is_live(k, index):
        bands = 4 >> k
        width = DMAX // bands
        first = 8 - (8 >> k)
        count = jnp.full((8, 128), live[first], jnp.int32)
        for band in range(1, bands):
            count = jnp.where(index // width == band, live[first + band], count)
        return (index & (width - 1)) < count

    for offset in range(CHIPS):
        block = lax.rem(z + offset, CHIPS) * 256 + core * ROWS
        packed[pl.ds(offset, 1), :] = entries(2, pl.multiple_of(block, 128))
    top = packed[...]
    middle = look_up(1, top >> 11)
    bottom = look_up(0, middle >> 11)
    late = (top & 2047) + (middle & 2047) + (bottom & 2047)
    row = (bottom >> 11) & 255
    start = (row >> 3) * SPAN + (row & 7) + OWN * 8 - (late >> 7) * 8
    start = jnp.where(is_live(1, top >> 11) & is_live(0, middle >> 11), start, ZERO_ROW + OWN * 8)
    packed[...] = start * 128 + (late & 127)
    to_scalar = pltpu.make_async_copy(packed, picks, table_sem.at[0])
    to_scalar.start()
    to_scalar.wait()

    @pl.when(tm > 0)
    def _():
        near.wait_recv()
        near_across.start()

    @pl.when(tm > 1)
    def _():
        far.wait_recv()
        far_across.start()

    to_partner.wait_recv()

    @pl.when(tm > 0)
    def _():
        near_across.wait_recv()

    @pl.when(tm > 1)
    def _():
        far_across.wait_recv()

    lanes = lax.broadcasted_iota(jnp.int32, (8, 128), 1)

    def contribution(offset, row):
        entry = picks[offset, row]
        start = entry >> 7
        shift = entry & 127
        same = flat[pl.ds(start, 8, stride=8), :]
        before = flat[pl.ds(start - 8, 8, stride=8), :]
        return pltpu.roll(jnp.where(lanes < 128 - shift, same, before), shift, 1)

    def message(direction, step, half, unit):
        return (direction * 4 + step) * 2 * HALF_UNITS + half * HALF_UNITS + unit

    def copy_of(direction, step, half, unit):
        index = message(direction, step, half, unit)
        return remote(
            sent.at[index], landed.at[index], send_sem.at[index], recv_sem.at[index],
            {"freq": ring[direction]},
        )

    def add_and_send(direction, step, half, unit):
        index = message(direction, step, half, unit)
        offset = 4 - step if direction == 0 else 4 + step
        first_row = half * 64 + unit * UNIT
        fresh = step == 0 or (step == 1 and half != direction)
        if not fresh:
            copy_of(direction, step - 1, half, unit).wait_recv()
        previous = message(direction, step - 1, half, unit)

        def body(i, carry):
            for k in range(8):
                row = i * 8 + k
                value = contribution(offset, first_row + row)
                at = pl.ds(pl.multiple_of(row * 8, 8), 8)
                if not fresh:
                    value = value + landed[previous, at, :]
                sent[index, at, :] = value
            return carry

        lax.fori_loop(0, UNIT // 8, body, 0)
        copy_of(direction, step, half, unit).start()

    messages = []
    for step in range(4):
        for turn in range(2):
            if step == 0 and turn == 0:
                continue
            for unit in range(HALF_UNITS):
                for direction in range(2):
                    half = direction if turn == 1 else 1 - direction
                    messages.append((direction, step, half, unit))
    for entry in messages:
        add_and_send(*entry)

    first_row = freq * ROWS
    for half in range(2):
        for unit in range(HALF_UNITS):
            incoming = []
            for direction in range(2):
                copy_of(direction, 3, half, unit).wait_recv()
                incoming.append(message(direction, 3, half, unit))

            def body(i, carry, half=half, unit=unit, incoming=incoming):
                for k in range(8):
                    row = i * 8 + k
                    local = half * 64 + unit * UNIT + row
                    at = pl.ds(pl.multiple_of(row * 8, 8), 8)
                    value = contribution(0, local) + landed[incoming[0], at, :] + landed[incoming[1], at, :]
                    alive = first_row + local < live[6]
                    value = jnp.where(alive, value, jnp.zeros_like(value))
                    place = (half * 64 + unit * UNIT) * 8 + i * 64 + k
                    out[pl.ds(place, 8, stride=8), :] = value
                return carry

            lax.fori_loop(0, UNIT // 8, body, 0)

    @pl.when(tm < tm_count - 1)
    def _():
        near.wait_send()

    @pl.when(tm < tm_count - 2)
    def _():
        far.wait_send()

    to_partner.wait_send()

    @pl.when(tm > 0)
    def _():
        near_across.wait_send()

    @pl.when(tm > 1)
    def _():
        far_across.wait_send()

    for entry in messages:
        copy_of(*entry).wait_send()


def per_device(band_state, lower_rows, upper_rows, delays, counts):
    tiles = band_state.reshape(16, 8, 8, 128).transpose(0, 2, 1, 3).reshape(16, 64, 128)
    message_count = 2 * 4 * 2 * HALF_UNITS
    dma = pltpu.SemaphoreType.DMA
    out = pl.pallas_call(
        kernel,
        out_shape=jax.ShapeDtypeStruct((1024, 128), jnp.float32),
        in_specs=[pl.BlockSpec(memory_space=pltpu.HBM)] * 5,
        out_specs=pl.BlockSpec(memory_space=pltpu.VMEM),
        scratch_shapes=[
            pltpu.VMEM((GROUPS + 1, SPAN, 128), jnp.float32),
            pltpu.VMEM((ITERS, DMAX), jnp.int32),
            pltpu.VMEM((ITERS, DMAX), jnp.int32),
            pltpu.VMEM((ITERS, DMAX), jnp.int32),
            pltpu.SMEM((7,), jnp.int32),
            pltpu.VMEM((CHIPS, ROWS), jnp.int32),
            pltpu.SMEM((CHIPS, ROWS), jnp.int32),
            pltpu.VMEM((message_count, UNIT * 8, 128), jnp.float32),
            pltpu.VMEM((message_count, UNIT * 8, 128), jnp.float32),
            dma,
            dma((4,)),
            dma((2,)),
            dma((2,)),
            dma((2,)),
            dma((4,)),
            dma((message_count,)),
            dma((message_count,)),
        ],
        compiler_params=pltpu.CompilerParams(collective_id=0, has_side_effects=True, vmem_limit_bytes=40 << 20),
    )(*(pltpu.with_memory_space_constraint(a, pltpu.HBM) for a in (tiles, lower_rows, upper_rows, delays, counts)))
    return out.reshape(16, 8, 8, 128).transpose(0, 2, 1, 3).reshape(ROWS, 1024)


def solution(mesh):
    return jax.shard_map(
        per_device,
        mesh=mesh,
        in_specs=(P("freq", "tm"), P(), P(), P(), P()),
        out_specs=P("freq", "tm"),
        check_vma=False,
    )
```

```python
import jax
import jax.numpy as jnp
from jax import lax
from jax.experimental import pallas as pl
from jax.experimental.pallas import tpu as pltpu
from jax.sharding import PartitionSpec as P

DMAX = 2048
ITERS = 3
MESH = pl.DeviceIdType.MESH

CHIPS = 8
ROWS = 128
GROUPS = 32
TILES = 23
SPAN = TILES * 8
SET = (GROUPS + 1) * SPAN
HERE = 11
SKEW = 4
PHASES = 2
WIDTH = 8 // PHASES
UNIT = 32
HALF_UNITS = 64 // UNIT
ZERO_ROW = GROUPS * SPAN

EARLY = SKEW + 8 - WIDTH - 14
FETCHES = [[(-1, 8 + EARLY, -EARLY), (1, 0, SKEW)]]
for phase in range(1, PHASES):
    last = EARLY - (phase - 1) * WIDTH
    first = last - WIDTH
    pieces = []
    if last > -8:
        pieces.append((-1, 8 + max(first, -8), last - max(first, -8)))
    if first < -8:
        pieces.append((-2, 16 + first, min(last, -8) - first))
    FETCHES.append(pieces)
LATE = [(phase, *piece) for phase in range(1, PHASES) for piece in FETCHES[phase]]


def kernel(
    x, lower, upper, delays, counts, out,
    raw, lower_table, upper_table, delay_table, live, packed, picks, sent, landed, late, shipped, received,
    local_sem, table_sem, own_sem, early_sem, late_sem, send_sem, recv_sem, ship_sem,
):
    freq = lax.axis_index("freq")
    tm = lax.axis_index("tm")
    tm_count = lax.axis_size("tm")
    z = lax.div(freq, 2)
    core = lax.rem(freq, 2)
    bits = [lax.rem(z, 2), lax.rem(lax.div(z, 2), 2), lax.div(z, 4)]
    partner = {"freq": freq + 1 - 2 * core}
    ring = ({"freq": lax.rem(freq + 2, 16)}, {"freq": lax.rem(freq + 14, 16)})
    flat = raw.reshape(2 * SET, 128)
    mine = pl.ds(core * 16, 16)

    def ahead(distance):
        return {"tm": lax.rem(tm + tm_count + distance, tm_count)}

    def tiles(first, count):
        return pl.ds((HERE + first) * 8, count * 8)

    own = pltpu.make_async_copy(x, raw.at[mine, tiles(0, 8), :], local_sem)
    own.start()
    tables = [
        pltpu.make_async_copy(source, target, table_sem.at[n])
        for n, (source, target) in enumerate(
            ((lower, lower_table), (upper, upper_table), (delays, delay_table), (counts, live))
        )
    ]
    for table in tables:
        table.start()

    barrier = pltpu.get_barrier_semaphore()
    peers = [partner, *ring, ahead(1), ahead(-1), ahead(2), ahead(-2)]
    for peer in peers:
        pl.semaphore_signal(barrier, inc=1, device_id=peer, device_id_type=MESH)
    pl.semaphore_wait(barrier, len(peers))

    own.wait()

    def remote(source, target, send, recv, device):
        return pltpu.make_async_remote_copy(
            src_ref=source, dst_ref=target, send_sem=send, recv_sem=recv,
            device_id=device, device_id_type=MESH,
        )

    def sends(distance):
        return tm < tm_count + distance if distance < 0 else tm >= 0

    def receives(distance):
        return tm >= -distance if distance < 0 else tm >= 0

    early = []
    for n, (distance, first, count) in enumerate(FETCHES[0]):
        place = raw.at[mine, tiles(distance * 8 + first, count), :]
        early.append((
            distance,
            remote(raw.at[mine, tiles(first, count), :], place, early_sem.at[4 * n], early_sem.at[4 * n + 1], ahead(-distance)),
            remote(place, place, early_sem.at[4 * n + 2], early_sem.at[4 * n + 3], partner),
        ))
    fetched = []
    for n, (phase, distance, first, count) in enumerate(LATE):
        place = late.at[n, mine, pl.ds(0, count * 8), :]
        fetched.append((
            phase, distance, distance * 8 + first, count,
            remote(raw.at[mine, tiles(first, count), :], place, late_sem.at[4 * n], late_sem.at[4 * n + 1], ahead(-distance)),
            remote(place, place, late_sem.at[4 * n + 2], late_sem.at[4 * n + 3], partner),
        ))
    to_partner = remote(
        raw.at[mine, tiles(0, 8), :], raw.at[mine, tiles(0, 8), :], own_sem.at[0], own_sem.at[1], partner
    )

    for distance, copy, _ in early:
        pl.when(sends(distance))(copy.start)
    for _, distance, _, _, copy, _ in fetched:
        pl.when(sends(distance))(copy.start)
    to_partner.start()

    def clear(base, first, count):
        def body(g, carry):
            raw[base + g, tiles(first, count), :] = jnp.zeros((count * 8, 128), jnp.float32)
            return carry
        lax.fori_loop(0, GROUPS, body, 0)

    raw[GROUPS, :, :] = jnp.zeros((SPAN, 128), jnp.float32)

    @pl.when(tm == 0)
    def _():
        clear(0, -10, 10)

    @pl.when(tm == 1)
    def _():
        clear(0, -10, 2)

    @pl.when(tm == tm_count - 1)
    def _():
        clear(GROUPS + 1, -HERE, HERE + 8)
        raw[2 * GROUPS + 1, :, :] = jnp.zeros((SPAN, 128), jnp.float32)

    for table in tables:
        table.wait()

    def entries(k, block):
        at = (pl.ds(k, 1), pl.ds(block, 128))
        row = jnp.where(bits[k] == 1, upper_table[at], lower_table[at])
        return row * 2048 + delay_table[at] * bits[k]

    def look_up(k, index):
        found = jnp.zeros((8, 128), jnp.int32)
        for block in range(DMAX // 128):
            table = jnp.broadcast_to(entries(k, block * 128), (8, 128))
            here = jnp.take_along_axis(table, index & 127, axis=1)
            found = jnp.where(index >> 7 == block, here, found)
        return found

    def is_live(k, index):
        bands = 4 >> k
        width = DMAX // bands
        first = 8 - (8 >> k)
        count = jnp.full((8, 128), live[first], jnp.int32)
        for band in range(1, bands):
            count = jnp.where(index // width == band, live[first + band], count)
        return (index & (width - 1)) < count

    for offset in range(CHIPS):
        block = lax.rem(z + offset, CHIPS) * 256 + core * ROWS
        packed[pl.ds(offset, 1), :] = entries(2, pl.multiple_of(block, 128))
    top = packed[...]
    middle = look_up(1, top >> 11)
    bottom = look_up(0, middle >> 11)
    delay = (top & 2047) + (middle & 2047) + (bottom & 2047)
    row = (bottom >> 11) & 255
    start = (row >> 3) * SPAN + (row & 7) + (HERE - (delay >> 7)) * 8
    start = jnp.where(is_live(1, top >> 11) & is_live(0, middle >> 11), start, ZERO_ROW + HERE * 8)
    packed[...] = start * 128 + (delay & 127)
    to_scalar = pltpu.make_async_copy(packed, picks, table_sem.at[0])
    to_scalar.start()
    to_scalar.wait()

    for distance, copy, across in early:
        @pl.when(receives(distance))
        def _(copy=copy, across=across):
            copy.wait_recv()
            across.start()
    to_partner.wait_recv()
    for distance, _, across in early:
        pl.when(receives(distance))(across.wait_recv)

    @pl.when(tm == tm_count - 1)
    def _():
        def body(g, carry):
            raw[GROUPS + 1 + g, tiles(8, SKEW), :] = raw[g, tiles(8, SKEW), :]
            return carry
        lax.fori_loop(0, GROUPS, body, 0)

    def forward(phase):
        for when, distance, _, _, copy, across in fetched:
            if when == phase:
                @pl.when(receives(distance))
                def _(copy=copy, across=across):
                    copy.wait_recv()
                    across.start()

    def settle(phase):
        for n, (when, distance, first, count, _, across) in enumerate(fetched):
            if when == phase:
                @pl.when(receives(distance))
                def _(n=n, first=first, count=count, across=across):
                    across.wait_recv()

                    def body(g, carry):
                        raw[g, tiles(first, count), :] = late[n, g, pl.ds(0, count * 8), :]
                        return carry
                    lax.fori_loop(0, GROUPS, body, 0)

    lanes = lax.broadcasted_iota(jnp.int32, (WIDTH, 128), 1)
    wrapped = jnp.where(tm == tm_count - 1, SET, 0)

    def first_tile(phase):
        return SKEW + 8 - (phase + 1) * WIDTH

    def contribution(phase, offset, row):
        entry = picks[offset, row]
        start = (entry >> 7) + first_tile(phase) * 8
        if first_tile(phase) >= 8:
            start = start + wrapped
        shift = entry & 127
        same = flat[pl.ds(start, WIDTH, stride=8), :]
        before = flat[pl.ds(start - 8, WIDTH, stride=8), :]
        return pltpu.roll(jnp.where(lanes < 128 - shift, same, before), shift, 1)

    def message(phase, direction, step, half, unit):
        return (((phase * 2 + direction) * 4 + step) * 2 + half) * HALF_UNITS + unit

    def copy_of(*entry):
        index = message(*entry)
        return remote(sent.at[index], landed.at[index], send_sem.at[index], recv_sem.at[index], ring[entry[1]])

    def add_and_send(phase, direction, step, half, unit):
        index = message(phase, direction, step, half, unit)
        offset = 4 - step if direction == 0 else 4 + step
        first_row = half * 64 + unit * UNIT
        fresh = step == 0 or (step == 1 and half != direction)
        previous = message(phase, direction, step - 1, half, unit)
        if not fresh:
            copy_of(phase, direction, step - 1, half, unit).wait_recv()

        def body(i, carry):
            for k in range(8):
                row = i * 8 + k
                value = contribution(phase, offset, first_row + row)
                at = pl.ds(pl.multiple_of(row * WIDTH, WIDTH), WIDTH)
                if not fresh:
                    value = value + landed[previous, at, :]
                sent[index, at, :] = value
            return carry

        lax.fori_loop(0, UNIT // 8, body, 0)
        copy_of(phase, direction, step, half, unit).start()

    def ship(phase, half, unit):
        index = (phase * 2 + half) * HALF_UNITS + unit
        return remote(shipped.at[index], received.at[index], ship_sem.at[0, index], ship_sem.at[1, index], ahead(1))

    def finish(phase, half, unit):
        incoming = []
        for direction in range(2):
            copy_of(phase, direction, 3, half, unit).wait_recv()
            incoming.append(message(phase, direction, 3, half, unit))
        first_row = half * 64 + unit * UNIT
        tile = first_tile(phase)
        index = (phase * 2 + half) * HALF_UNITS + unit

        def body(i, carry):
            for k in range(8):
                row = i * 8 + k
                at = pl.ds(pl.multiple_of(row * WIDTH, WIDTH), WIDTH)
                value = contribution(phase, 0, first_row + row)
                value = value + landed[incoming[0], at, :] + landed[incoming[1], at, :]
                alive = freq * ROWS + first_row + row < live[6]
                value = jnp.where(alive, value, jnp.zeros_like(value))
                if tile >= 8:
                    shipped[index, pl.ds(i * WIDTH * 8 + k, WIDTH, stride=8), :] = value
                else:
                    out[pl.ds(first_row * 8 + i * 64 + tile * 8 + k, WIDTH, stride=8), :] = value
            return carry

        lax.fori_loop(0, UNIT // 8, body, 0)
        if tile >= 8:
            ship(phase, half, unit).start()

    def take(phase, half, unit):
        ship(phase, half, unit).wait_recv()
        index = (phase * 2 + half) * HALF_UNITS + unit
        first = half * 64 + unit * UNIT
        tile = first_tile(phase) - 8
        for group in range(UNIT // 8):
            rows = pl.ds(group * WIDTH * 8, WIDTH * 8)
            out[pl.ds(first * 8 + group * 64 + tile * 8, WIDTH * 8), :] = received[index, rows, :]

    def exchange(phase, step, turn):
        for unit in range(HALF_UNITS):
            for direction in range(2):
                half = direction if turn == 1 else 1 - direction
                messages.append((phase, direction, step, half, unit))
                add_and_send(*messages[-1])

    parts = [(half, unit) for half in range(2) for unit in range(HALF_UNITS)]
    messages = []
    for phase in range(PHASES):
        if phase > 0:
            settle(phase)
        exchange(phase, 0, 1)
        exchange(phase, 1, 0)
        if phase > 0:
            for part in parts:
                finish(phase - 1, *part)
        exchange(phase, 1, 1)
        if phase + 1 < PHASES:
            forward(phase + 1)
        exchange(phase, 2, 0)
        exchange(phase, 2, 1)
        exchange(phase, 3, 0)
        exchange(phase, 3, 1)
    shipments = [(phase, *part) for phase in range(PHASES) if first_tile(phase) >= 8 for part in parts]
    for shipment in shipments:
        if shipment[0] < PHASES - 1:
            take(*shipment)
    for part in parts:
        finish(PHASES - 1, *part)

    for distance, copy, across in early:
        pl.when(sends(distance))(copy.wait_send)
        pl.when(receives(distance))(across.wait_send)
    for _, distance, _, _, copy, across in fetched:
        pl.when(sends(distance))(copy.wait_send)
        pl.when(receives(distance))(across.wait_send)
    to_partner.wait_send()
    for entry in messages:
        copy_of(*entry).wait_send()
    for shipment in shipments:
        ship(*shipment).wait_send()


def per_device(band_state, lower_rows, upper_rows, delays, counts):
    blocks = band_state.reshape(16, 8, 8, 128).transpose(0, 2, 1, 3).reshape(16, 64, 128)
    message_count = PHASES * 2 * 4 * 2 * HALF_UNITS
    part_count = PHASES * 2 * HALF_UNITS
    late_tiles = max(piece[3] for piece in LATE)
    operands = (blocks, lower_rows, upper_rows, delays, counts)
    dma = pltpu.SemaphoreType.DMA
    out = pl.pallas_call(
        kernel,
        out_shape=jax.ShapeDtypeStruct((1024, 128), jnp.float32),
        in_specs=[pl.BlockSpec(memory_space=pltpu.HBM)] * 5,
        out_specs=pl.BlockSpec(memory_space=pltpu.VMEM),
        scratch_shapes=[
            pltpu.VMEM((2 * (GROUPS + 1), SPAN, 128), jnp.float32),
            pltpu.VMEM((ITERS, DMAX), jnp.int32),
            pltpu.VMEM((ITERS, DMAX), jnp.int32),
            pltpu.VMEM((ITERS, DMAX), jnp.int32),
            pltpu.SMEM((7,), jnp.int32),
            pltpu.VMEM((CHIPS, ROWS), jnp.int32),
            pltpu.SMEM((CHIPS, ROWS), jnp.int32),
            pltpu.VMEM((message_count, UNIT * WIDTH, 128), jnp.float32),
            pltpu.VMEM((message_count, UNIT * WIDTH, 128), jnp.float32),
            pltpu.VMEM((len(LATE), GROUPS, late_tiles * 8, 128), jnp.float32),
            pltpu.VMEM((part_count, UNIT * WIDTH, 128), jnp.float32),
            pltpu.VMEM((part_count, UNIT * WIDTH, 128), jnp.float32),
            dma,
            dma((4,)),
            dma((2,)),
            dma((8,)),
            dma((4 * len(LATE),)),
            dma((message_count,)),
            dma((message_count,)),
            dma((2, part_count)),
        ],
        compiler_params=pltpu.CompilerParams(collective_id=0, has_side_effects=True, vmem_limit_bytes=48 << 20),
    )(*(pltpu.with_memory_space_constraint(operand, pltpu.HBM) for operand in operands))
    return out.reshape(16, 8, 8, 128).transpose(0, 2, 1, 3).reshape(ROWS, 1024)


def solution(mesh):
    return jax.shard_map(
        per_device,
        mesh=mesh,
        in_specs=(P("freq", "tm"), P(), P(), P(), P()),
        out_specs=P("freq", "tm"),
        check_vma=False,
    )
```

```python
import jax
import jax.numpy as jnp
from jax import lax
from jax.experimental import pallas as pl
from jax.experimental.pallas import tpu as pltpu
from jax.sharding import PartitionSpec as P

DMAX = 2048
ITERS = 3
MESH = pl.DeviceIdType.MESH

CHIPS = 8
ROWS = 128
GROUPS = 32
TILES = 23
SPAN = TILES * 8
SET = (GROUPS + 1) * SPAN
HERE = 11
SKEW = 4
UNIT = 64
UNITS = ROWS // UNIT
FINISH_ORDER = [unit + side * UNITS // 2 for unit in range(UNITS // 2) for side in range(2)]
ZERO_ROW = GROUPS * SPAN
PHASES = ((10, 2), (8, 2), (4, 4))
PARTS = 1

FETCHES = (((-1, 4, 4), (1, 0, 4)), ((-1, 2, 2),), ((-1, 0, 2), (-2, 6, 2)))
LATE = tuple((phase, *piece) for phase in range(1, len(PHASES)) for piece in FETCHES[phase])
LATE_TILES = max(piece[3] for piece in LATE)

MESSAGE_ROWS = [sum(2 * 4 * ROWS * width for _, width in PHASES[:phase]) for phase in range(len(PHASES) + 1)]
RESULT_ROWS = [sum(ROWS * width for _, width in PHASES[:phase]) for phase in range(len(PHASES) + 1)]


def kernel(
    x, lower, upper, delays, counts, out,
    raw, lower_table, upper_table, delay_table, live, packed, picks, sent, landed, late, shipped, received, partial,
    local_sem, table_sem, own_sem, early_sem, late_sem, send_sem, recv_sem, ship_sem,
):
    freq = lax.axis_index("freq")
    tm = lax.axis_index("tm")
    tm_count = lax.axis_size("tm")
    z = lax.div(freq, 2)
    core = lax.rem(freq, 2)
    bits = [lax.rem(z, 2), lax.rem(lax.div(z, 2), 2), lax.div(z, 4)]
    partner = {"freq": freq + 1 - 2 * core}
    ring = ({"freq": lax.rem(freq + 2, 16)}, {"freq": lax.rem(freq + 14, 16)})
    flat = raw.reshape(2 * SET, 128)
    mine = pl.ds(core * 16, 16)

    def ahead(distance):
        return {"tm": lax.rem(tm + tm_count + distance, tm_count)}

    def tiles(first, count):
        return pl.ds((HERE + first) * 8, count * 8)

    own = pltpu.make_async_copy(x, raw.at[mine, tiles(0, 8), :], local_sem)
    own.start()
    tables = [
        pltpu.make_async_copy(source, target, table_sem.at[n])
        for n, (source, target) in enumerate(
            ((lower, lower_table), (upper, upper_table), (delays, delay_table), (counts, live))
        )
    ]
    for table in tables:
        table.start()

    barrier = pltpu.get_barrier_semaphore()
    peers = [partner, *ring, ahead(1), ahead(-1), ahead(2), ahead(-2)]
    for peer in peers:
        pl.semaphore_signal(barrier, inc=1, device_id=peer, device_id_type=MESH)
    pl.semaphore_wait(barrier, len(peers))

    own.wait()

    def remote(source, target, send, recv, device):
        return pltpu.make_async_remote_copy(
            src_ref=source, dst_ref=target, send_sem=send, recv_sem=recv,
            device_id=device, device_id_type=MESH,
        )

    def sends(distance):
        return tm < tm_count + distance if distance < 0 else tm >= 0

    def receives(distance):
        return tm >= -distance if distance < 0 else tm >= 0

    size = 16 // PARTS
    shares = [pl.ds(core * 16 + part * size, size) for part in range(PARTS)]
    early = []
    for distance, first, count in FETCHES[0]:
        for share in shares:
            place = raw.at[share, tiles(distance * 8 + first, count), :]
            n = 4 * len(early)
            early.append((
                distance,
                remote(raw.at[share, tiles(first, count), :], place, early_sem.at[n], early_sem.at[n + 1], ahead(-distance)),
                remote(place, place, early_sem.at[n + 2], early_sem.at[n + 3], partner),
            ))
    early = [entry for part in range(PARTS) for entry in early[part::PARTS]]
    fetched = []
    for n, (phase, distance, first, count) in enumerate(LATE):
        place = late.at[n, mine, pl.ds(0, count * 8), :]
        fetched.append((
            phase, distance, distance * 8 + first, count,
            remote(raw.at[mine, tiles(first, count), :], place, late_sem.at[4 * n], late_sem.at[4 * n + 1], ahead(-distance)),
            remote(place, place, late_sem.at[4 * n + 2], late_sem.at[4 * n + 3], partner),
        ))
    to_partner = remote(
        raw.at[mine, tiles(0, 8), :], raw.at[mine, tiles(0, 8), :], own_sem.at[0], own_sem.at[1], partner
    )

    for distance, copy, _ in early:
        pl.when(sends(distance))(copy.start)
    for _, distance, _, _, copy, _ in fetched:
        pl.when(sends(distance))(copy.start)
    to_partner.start()

    def clear(base, first, count):
        def body(g, carry):
            raw[base + g, tiles(first, count), :] = jnp.zeros((count * 8, 128), jnp.float32)
            return carry
        lax.fori_loop(0, GROUPS, body, 0)

    raw[GROUPS, :, :] = jnp.zeros((SPAN, 128), jnp.float32)

    @pl.when(tm == 0)
    def _():
        clear(0, -10, 10)

    @pl.when(tm == 1)
    def _():
        clear(0, -10, 2)

    @pl.when(tm == tm_count - 1)
    def _():
        clear(GROUPS + 1, -HERE, HERE + 8)
        raw[2 * GROUPS + 1, :, :] = jnp.zeros((SPAN, 128), jnp.float32)

    for table in tables:
        table.wait()

    def entries(k, block):
        at = (pl.ds(k, 1), pl.ds(block, 128))
        row = jnp.where(bits[k] == 1, upper_table[at], lower_table[at])
        return row * 2048 + delay_table[at] * bits[k]

    def look_up(k, index):
        found = jnp.zeros((8, 128), jnp.int32)
        for block in range(DMAX // 128):
            table = jnp.broadcast_to(entries(k, block * 128), (8, 128))
            here = jnp.take_along_axis(table, index & 127, axis=1)
            found = jnp.where(index >> 7 == block, here, found)
        return found

    def is_live(k, index):
        bands = 4 >> k
        width = DMAX // bands
        first = 8 - (8 >> k)
        count = jnp.full((8, 128), live[first], jnp.int32)
        for band in range(1, bands):
            count = jnp.where(index // width == band, live[first + band], count)
        return (index & (width - 1)) < count

    for offset in range(CHIPS):
        block = lax.rem(z + offset, CHIPS) * 256 + core * ROWS
        packed[pl.ds(offset, 1), :] = entries(2, pl.multiple_of(block, 128))
    top = packed[...]
    middle = look_up(1, top >> 11)
    bottom = look_up(0, middle >> 11)
    delay = (top & 2047) + (middle & 2047) + (bottom & 2047)
    row = (bottom >> 11) & 255
    start = (row >> 3) * SPAN + (row & 7) + (HERE - (delay >> 7)) * 8
    start = jnp.where(is_live(1, top >> 11) & is_live(0, middle >> 11), start, ZERO_ROW + HERE * 8)
    packed[...] = start * 128 + (delay & 127)
    to_scalar = pltpu.make_async_copy(packed, picks, table_sem.at[0])
    to_scalar.start()
    to_scalar.wait()

    for distance, copy, across in early:
        @pl.when(receives(distance))
        def _(copy=copy, across=across):
            copy.wait_recv()
            across.start()
    to_partner.wait_recv()
    for distance, _, across in early:
        pl.when(receives(distance))(across.wait_recv)

    @pl.when(tm == tm_count - 1)
    def _():
        def body(g, carry):
            raw[GROUPS + 1 + g, tiles(8, SKEW), :] = raw[g, tiles(8, SKEW), :]
            return carry
        lax.fori_loop(0, GROUPS, body, 0)

    def forward(phase):
        for when, distance, _, _, copy, across in fetched:
            if when == phase:
                @pl.when(receives(distance))
                def _(copy=copy, across=across):
                    copy.wait_recv()
                    across.start()

    def settle(phase):
        for n, (when, distance, first, count, _, across) in enumerate(fetched):
            if when == phase:
                @pl.when(receives(distance))
                def _(n=n, first=first, count=count, across=across):
                    across.wait_recv()

                    def body(g, carry):
                        raw[g, tiles(first, count), :] = late[n, g, pl.ds(0, count * 8), :]
                        return carry
                    lax.fori_loop(0, GROUPS, body, 0)

    wrapped = jnp.where(tm == tm_count - 1, SET, 0)

    def contribution(phase, offset, row):
        tile, width = PHASES[phase]
        entry = picks[offset, row]
        start = (entry >> 7) + tile * 8
        if tile >= 8:
            start = start + wrapped
        shift = entry & 127
        same = flat[pl.ds(start, width, stride=8), :]
        before = flat[pl.ds(start - 8, width, stride=8), :]
        lanes = lax.broadcasted_iota(jnp.int32, (width, 128), 1)
        return pltpu.roll(jnp.where(lanes < 128 - shift, same, before), shift, 1)

    def first_row(phase, direction, step, unit):
        return MESSAGE_ROWS[phase] + ((direction * 4 + step) * UNITS + unit) * UNIT * PHASES[phase][1]

    def copy_of(phase, direction, step, unit):
        rows = pl.ds(first_row(phase, direction, step, unit), UNIT * PHASES[phase][1])
        n = ((phase * 2 + direction) * 4 + step) * UNITS + unit
        return remote(sent.at[rows, :], landed.at[rows, :], send_sem.at[n], recv_sem.at[n], ring[direction])

    def is_long(direction, unit):
        return (unit < UNITS // 2) == (direction == 0)

    messages = []

    def add_and_send(phase, direction, step, unit, fresh):
        width = PHASES[phase][1]
        offset = 4 - step if direction == 0 else 4 + step
        target = first_row(phase, direction, step, unit)
        source = first_row(phase, direction, step - 1, unit)
        if not fresh:
            copy_of(phase, direction, step - 1, unit).wait_recv()

        for row in range(UNIT):
            value = contribution(phase, offset, unit * UNIT + row)
            if not fresh:
                value = value + landed[pl.ds(source + row * width, width), :]
            sent[pl.ds(target + row * width, width), :] = value
        copy_of(phase, direction, step, unit).start()
        messages.append((phase, direction, step, unit))

    def exchange(phase, step, long, fresh):
        for unit in range(UNITS):
            for direction in range(2):
                if is_long(direction, unit) == long:
                    add_and_send(phase, direction, step, unit, fresh)

    def begin(phase):
        exchange(phase, 0, True, True)
        exchange(phase, 1, False, True)

    def go_on(phase, step):
        if step > 1:
            exchange(phase, step, False, False)
        exchange(phase, step, True, False)

    def ship(phase, unit):
        width = PHASES[phase][1]
        rows = pl.ds(RESULT_ROWS[phase] + unit * UNIT * width, UNIT * width)
        n = phase * UNITS + unit
        return remote(shipped.at[rows, :], received.at[rows, :], ship_sem.at[0, n], ship_sem.at[1, n], ahead(1))

    def finish(phase):
        tile, width = PHASES[phase]
        for unit in FINISH_ORDER:
            sources = [first_row(phase, direction, 3, unit) for direction in range(2)]
            last = 0 if is_long(0, unit) else 1
            copy_of(phase, 1 - last, 3, unit).wait_recv()
            for row in range(UNIT):
                value = contribution(phase, 0, unit * UNIT + row)
                value = value + landed[pl.ds(sources[1 - last] + row * width, width), :]
                alive = freq * ROWS + unit * UNIT + row < live[6]
                partial[pl.ds(row * width, width), :] = jnp.where(alive, value, jnp.zeros_like(value))
            copy_of(phase, last, 3, unit).wait_recv()
            for row in range(UNIT):
                alive = freq * ROWS + unit * UNIT + row < live[6]
                value = landed[pl.ds(sources[last] + row * width, width), :]
                value = partial[pl.ds(row * width, width), :] + jnp.where(alive, value, jnp.zeros_like(value))
                if tile >= 8:
                    at = RESULT_ROWS[phase] + unit * UNIT * width + (row // 8) * width * 8 + row % 8
                    shipped[pl.ds(at, width, stride=8), :] = value
                else:
                    out[pl.ds((unit * UNIT + row - row % 8) * 8 + tile * 8 + row % 8, width, stride=8), :] = value
            if tile >= 8:
                ship(phase, unit).start()

    def take(phase):
        tile, width = PHASES[phase]
        for unit in range(UNITS):
            ship(phase, unit).wait_recv()
            for group in range(UNIT // 8):
                rows = pl.ds(RESULT_ROWS[phase] + (unit * UNIT + group * 8) * width, 8 * width)
                out[pl.ds(unit * UNIT * 8 + group * 64 + (tile - 8) * 8, 8 * width), :] = received[rows, :]

    begin(0)
    forward(1)
    settle(1)
    begin(1)
    go_on(0, 1)
    go_on(1, 1)
    forward(2)
    go_on(0, 2)
    go_on(1, 2)
    go_on(0, 3)
    settle(2)
    begin(2)
    go_on(1, 3)
    finish(0)
    go_on(2, 1)
    finish(1)
    go_on(2, 2)
    take(0)
    go_on(2, 3)
    take(1)
    finish(2)

    for distance, copy, across in early:
        pl.when(sends(distance))(copy.wait_send)
        pl.when(receives(distance))(across.wait_send)
    for _, distance, _, _, copy, across in fetched:
        pl.when(sends(distance))(copy.wait_send)
        pl.when(receives(distance))(across.wait_send)
    to_partner.wait_send()
    for entry in messages:
        copy_of(*entry).wait_send()
    for phase, (tile, _) in enumerate(PHASES):
        if tile >= 8:
            for unit in range(UNITS):
                ship(phase, unit).wait_send()


def per_device(band_state, lower_rows, upper_rows, delays, counts):
    blocks = band_state.reshape(16, 8, 8, 128).transpose(0, 2, 1, 3).reshape(16, 64, 128)
    message_count = len(PHASES) * 2 * 4 * UNITS
    operands = (blocks, lower_rows, upper_rows, delays, counts)
    dma = pltpu.SemaphoreType.DMA
    out = pl.pallas_call(
        kernel,
        out_shape=jax.ShapeDtypeStruct((1024, 128), jnp.float32),
        in_specs=[pl.BlockSpec(memory_space=pltpu.HBM)] * 5,
        out_specs=pl.BlockSpec(memory_space=pltpu.VMEM),
        scratch_shapes=[
            pltpu.VMEM((2 * (GROUPS + 1), SPAN, 128), jnp.float32),
            pltpu.VMEM((ITERS, DMAX), jnp.int32),
            pltpu.VMEM((ITERS, DMAX), jnp.int32),
            pltpu.VMEM((ITERS, DMAX), jnp.int32),
            pltpu.SMEM((7,), jnp.int32),
            pltpu.VMEM((CHIPS, ROWS), jnp.int32),
            pltpu.SMEM((CHIPS, ROWS), jnp.int32),
            pltpu.VMEM((MESSAGE_ROWS[-1], 128), jnp.float32),
            pltpu.VMEM((MESSAGE_ROWS[-1], 128), jnp.float32),
            pltpu.VMEM((len(LATE), GROUPS, LATE_TILES * 8, 128), jnp.float32),
            pltpu.VMEM((RESULT_ROWS[-1], 128), jnp.float32),
            pltpu.VMEM((RESULT_ROWS[-1], 128), jnp.float32),
            pltpu.VMEM((UNIT * max(width for _, width in PHASES), 128), jnp.float32),
            dma,
            dma((4,)),
            dma((2,)),
            dma((4 * PARTS * len(FETCHES[0]),)),
            dma((4 * len(LATE),)),
            dma((message_count,)),
            dma((message_count,)),
            dma((2, len(PHASES) * UNITS)),
        ],
        compiler_params=pltpu.CompilerParams(collective_id=0, has_side_effects=True, vmem_limit_bytes=48 << 20),
    )(*(pltpu.with_memory_space_constraint(operand, pltpu.HBM) for operand in operands))
    return out.reshape(16, 8, 8, 128).transpose(0, 2, 1, 3).reshape(ROWS, 1024)


def solution(mesh):
    return jax.shard_map(
        per_device,
        mesh=mesh,
        in_specs=(P("freq", "tm"), P(), P(), P(), P()),
        out_specs=P("freq", "tm"),
        check_vma=False,
    )
```

```python
import jax
import jax.numpy as jnp
from jax import lax
from jax.experimental import pallas as pl
from jax.experimental.pallas import tpu as pltpu
from jax.sharding import PartitionSpec as P

DMAX = 2048
ITERS = 3
MESH = pl.DeviceIdType.MESH

CHIPS = 8
ROWS = 128
GROUPS = 32
TILES = 23
SPAN = TILES * 8
SET = (GROUPS + 1) * SPAN
HERE = 11
SKEW = 4
UNIT = 64
UNITS = ROWS // UNIT
FINISH_ORDER = [unit + side * UNITS // 2 for unit in range(UNITS // 2) for side in range(2)]
ZERO_ROW = GROUPS * SPAN
PHASES = ((10, 2), (8, 2), (4, 4))
PARTS = 1

FETCHES = (((-1, 4, 4), (1, 0, 4)), ((-1, 2, 2),), ((-1, 0, 2), (-2, 6, 2)))
LATE = tuple((phase, *piece) for phase in range(1, len(PHASES)) for piece in FETCHES[phase])
LATE_TILES = max(piece[3] for piece in LATE)

MESSAGE_ROWS = [sum(2 * 4 * ROWS * width for _, width in PHASES[:phase]) for phase in range(len(PHASES) + 1)]
RESULT_ROWS = [sum(ROWS * width for _, width in PHASES[:phase]) for phase in range(len(PHASES) + 1)]


def kernel(
    x, lower, upper, delays, counts, out,
    raw, lower_table, upper_table, delay_table, live, packed, picks, sent, landed, late, shipped, received, partial,
    local_sem, table_sem, own_sem, early_sem, late_sem, send_sem, recv_sem, ship_sem,
):
    freq = lax.axis_index("freq")
    tm = lax.axis_index("tm")
    tm_count = lax.axis_size("tm")
    z = lax.div(freq, 2)
    core = lax.rem(freq, 2)
    bits = [lax.rem(z, 2), lax.rem(lax.div(z, 2), 2), lax.div(z, 4)]
    partner = {"freq": freq + 1 - 2 * core}
    ring = ({"freq": lax.rem(freq + 2, 16)}, {"freq": lax.rem(freq + 14, 16)})
    flat = raw.reshape(2 * SET, 128)
    mine = pl.ds(core * 16, 16)

    def ahead(distance):
        return {"tm": lax.rem(tm + tm_count + distance, tm_count)}

    def tiles(first, count):
        return pl.ds((HERE + first) * 8, count * 8)

    own = pltpu.make_async_copy(x, raw.at[mine, tiles(0, 8), :], local_sem)
    own.start()
    tables = [
        pltpu.make_async_copy(source, target, table_sem.at[n])
        for n, (source, target) in enumerate(
            ((lower, lower_table), (upper, upper_table), (delays, delay_table), (counts, live))
        )
    ]
    for table in tables:
        table.start()

    barrier = pltpu.get_barrier_semaphore()
    peers = [partner, *ring, ahead(1), ahead(-1), ahead(2), ahead(-2)]
    for peer in peers:
        pl.semaphore_signal(barrier, inc=1, device_id=peer, device_id_type=MESH)
    pl.semaphore_wait(barrier, len(peers))

    own.wait()

    def remote(source, target, send, recv, device):
        return pltpu.make_async_remote_copy(
            src_ref=source, dst_ref=target, send_sem=send, recv_sem=recv,
            device_id=device, device_id_type=MESH,
        )

    def sends(distance):
        return tm < tm_count + distance if distance < 0 else tm >= 0

    def receives(distance):
        return tm >= -distance if distance < 0 else tm >= 0

    def first_chip(phase, tile):
        return (PHASES[phase][0] - tile) // 2 + 1

    size = 16 // PARTS
    shares = [pl.ds(core * 16 + part * size, size) for part in range(PARTS)]
    early = []
    for distance, first, count in FETCHES[0]:
        for share in shares:
            place = raw.at[share, tiles(distance * 8 + first, count), :]
            n = 4 * len(early)
            early.append((
                distance,
                remote(raw.at[share, tiles(first, count), :], place, early_sem.at[n], early_sem.at[n + 1], ahead(-distance)),
                remote(place, place, early_sem.at[n + 2], early_sem.at[n + 3], partner),
            ))
    early = [entry for part in range(PARTS) for entry in early[part::PARTS]]
    fetched = []
    for n, (phase, distance, first, count) in enumerate(LATE):
        place = late.at[n, mine, pl.ds(0, count * 8), :]
        fetched.append((
            phase, distance, distance * 8 + first, count,
            remote(raw.at[mine, tiles(first, count), :], place, late_sem.at[4 * n], late_sem.at[4 * n + 1], ahead(-distance)),
            remote(place, place, late_sem.at[4 * n + 2], late_sem.at[4 * n + 3], partner),
        ))
    to_partner = remote(
        raw.at[mine, tiles(0, 8), :], raw.at[mine, tiles(0, 8), :], own_sem.at[0], own_sem.at[1], partner
    )

    def reads_early(distance):
        return z >= first_chip(len(PHASES) - 1, 0) if distance < 0 else z >= 0

    for distance, copy, _ in early:
        pl.when(sends(distance) & reads_early(distance))(copy.start)
    def is_needed(first, count):
        return z >= first_chip(len(PHASES) - 1, first + count)

    for _, distance, first, count, copy, _ in fetched:
        pl.when(sends(distance) & is_needed(first, count))(copy.start)
    to_partner.start()

    def clear(base, first, count):
        def body(g, carry):
            raw[base + g, tiles(first, count), :] = jnp.zeros((count * 8, 128), jnp.float32)
            return carry
        lax.fori_loop(0, GROUPS, body, 0)

    raw[GROUPS, :, :] = jnp.zeros((SPAN, 128), jnp.float32)

    @pl.when(tm == 0)
    def _():
        clear(0, -10, 10)

    @pl.when(tm == 1)
    def _():
        clear(0, -10, 2)

    @pl.when(tm == tm_count - 1)
    def _():
        clear(GROUPS + 1, -HERE, HERE + 8)
        raw[2 * GROUPS + 1, :, :] = jnp.zeros((SPAN, 128), jnp.float32)

    for table in tables:
        table.wait()

    def entries(k, block):
        at = (pl.ds(k, 1), pl.ds(block, 128))
        row = jnp.where(bits[k] == 1, upper_table[at], lower_table[at])
        return row * 2048 + delay_table[at] * bits[k]

    def look_up(k, index):
        found = jnp.zeros((8, 128), jnp.int32)
        for block in range(DMAX // 128):
            table = jnp.broadcast_to(entries(k, block * 128), (8, 128))
            here = jnp.take_along_axis(table, index & 127, axis=1)
            found = jnp.where(index >> 7 == block, here, found)
        return found

    def is_live(k, index):
        bands = 4 >> k
        width = DMAX // bands
        first = 8 - (8 >> k)
        count = jnp.full((8, 128), live[first], jnp.int32)
        for band in range(1, bands):
            count = jnp.where(index // width == band, live[first + band], count)
        return (index & (width - 1)) < count

    for offset in range(CHIPS):
        block = lax.rem(z + offset, CHIPS) * 256 + core * ROWS
        packed[pl.ds(offset, 1), :] = entries(2, pl.multiple_of(block, 128))
    top = packed[...]
    middle = look_up(1, top >> 11)
    bottom = look_up(0, middle >> 11)
    delay = (top & 2047) + (middle & 2047) + (bottom & 2047)
    row = (bottom >> 11) & 255
    start = (row >> 3) * SPAN + (row & 7) + (HERE - (delay >> 7)) * 8
    start = jnp.where(is_live(1, top >> 11) & is_live(0, middle >> 11), start, ZERO_ROW + HERE * 8)
    packed[...] = start * 128 + (delay & 127)
    to_scalar = pltpu.make_async_copy(packed, picks, table_sem.at[0])
    to_scalar.start()
    to_scalar.wait()

    for distance, copy, across in early:
        @pl.when(receives(distance) & reads_early(distance))
        def _(copy=copy, across=across):
            copy.wait_recv()
            across.start()
    to_partner.wait_recv()
    for distance, _, across in early:
        pl.when(receives(distance) & reads_early(distance))(across.wait_recv)

    @pl.when(tm == tm_count - 1)
    def _():
        def body(g, carry):
            raw[GROUPS + 1 + g, tiles(8, SKEW), :] = raw[g, tiles(8, SKEW), :]
            return carry
        lax.fori_loop(0, GROUPS, body, 0)

    def when_first_read(phase, distance, first, count):
        here = receives(distance) & (z >= first_chip(phase, first + count))
        return here & (z < first_chip(phase - 1, first + count)) if phase > 1 else here

    def forward(phase):
        for when, distance, first, count, copy, across in fetched:
            if when <= phase:
                @pl.when(when_first_read(phase, distance, first, count))
                def _(copy=copy, across=across):
                    copy.wait_recv()
                    across.start()

    def settle(phase):
        for n, (when, distance, first, count, _, across) in enumerate(fetched):
            if when <= phase:
                @pl.when(when_first_read(phase, distance, first, count))
                def _(n=n, first=first, count=count, across=across):
                    across.wait_recv()

                    def body(g, carry):
                        raw[g, tiles(first, count), :] = late[n, g, pl.ds(0, count * 8), :]
                        return carry
                    lax.fori_loop(0, GROUPS, body, 0)

    wrapped = jnp.where(tm == tm_count - 1, SET, 0)

    def contribution(phase, offset, row):
        tile, width = PHASES[phase]
        entry = picks[offset, row]
        start = (entry >> 7) + tile * 8
        if tile >= 8:
            start = start + wrapped
        shift = entry & 127
        same = flat[pl.ds(start, width, stride=8), :]
        before = flat[pl.ds(start - 8, width, stride=8), :]
        lanes = lax.broadcasted_iota(jnp.int32, (width, 128), 1)
        return pltpu.roll(jnp.where(lanes < 128 - shift, same, before), shift, 1)

    def first_row(phase, direction, step, unit):
        return MESSAGE_ROWS[phase] + ((direction * 4 + step) * UNITS + unit) * UNIT * PHASES[phase][1]

    def copy_of(phase, direction, step, unit):
        rows = pl.ds(first_row(phase, direction, step, unit), UNIT * PHASES[phase][1])
        n = ((phase * 2 + direction) * 4 + step) * UNITS + unit
        return remote(sent.at[rows, :], landed.at[rows, :], send_sem.at[n], recv_sem.at[n], ring[direction])

    def is_long(direction, unit):
        return (unit < UNITS // 2) == (direction == 0)

    messages = []

    def add_and_send(phase, direction, step, unit, fresh):
        width = PHASES[phase][1]
        offset = 4 - step if direction == 0 else 4 + step
        target = first_row(phase, direction, step, unit)
        source = first_row(phase, direction, step - 1, unit)
        if not fresh:
            copy_of(phase, direction, step - 1, unit).wait_recv()

        for row in range(UNIT):
            value = contribution(phase, offset, unit * UNIT + row)
            if not fresh:
                value = value + landed[pl.ds(source + row * width, width), :]
            sent[pl.ds(target + row * width, width), :] = value
        copy_of(phase, direction, step, unit).start()
        messages.append((phase, direction, step, unit))

    def exchange(phase, step, long, fresh):
        for unit in range(UNITS):
            for direction in range(2):
                if is_long(direction, unit) == long:
                    add_and_send(phase, direction, step, unit, fresh)

    def begin(phase):
        exchange(phase, 0, True, True)
        exchange(phase, 1, False, True)

    def go_on(phase, step):
        if step > 1:
            exchange(phase, step, False, False)
        exchange(phase, step, True, False)

    def ship(phase, unit):
        width = PHASES[phase][1]
        rows = pl.ds(RESULT_ROWS[phase] + unit * UNIT * width, UNIT * width)
        n = phase * UNITS + unit
        return remote(shipped.at[rows, :], received.at[rows, :], ship_sem.at[0, n], ship_sem.at[1, n], ahead(1))

    def finish(phase):
        tile, width = PHASES[phase]
        for unit in FINISH_ORDER:
            sources = [first_row(phase, direction, 3, unit) for direction in range(2)]
            last = 0 if is_long(0, unit) else 1
            copy_of(phase, 1 - last, 3, unit).wait_recv()
            for row in range(UNIT):
                value = contribution(phase, 0, unit * UNIT + row)
                value = value + landed[pl.ds(sources[1 - last] + row * width, width), :]
                alive = freq * ROWS + unit * UNIT + row < live[6]
                partial[pl.ds(row * width, width), :] = jnp.where(alive, value, jnp.zeros_like(value))
            copy_of(phase, last, 3, unit).wait_recv()
            for row in range(UNIT):
                alive = freq * ROWS + unit * UNIT + row < live[6]
                value = landed[pl.ds(sources[last] + row * width, width), :]
                value = partial[pl.ds(row * width, width), :] + jnp.where(alive, value, jnp.zeros_like(value))
                if tile >= 8:
                    at = RESULT_ROWS[phase] + unit * UNIT * width + (row // 8) * width * 8 + row % 8
                    shipped[pl.ds(at, width, stride=8), :] = value
                else:
                    out[pl.ds((unit * UNIT + row - row % 8) * 8 + tile * 8 + row % 8, width, stride=8), :] = value
            if tile >= 8:
                ship(phase, unit).start()

    def take(phase):
        tile, width = PHASES[phase]
        for unit in range(UNITS):
            ship(phase, unit).wait_recv()
            for group in range(UNIT // 8):
                rows = pl.ds(RESULT_ROWS[phase] + (unit * UNIT + group * 8) * width, 8 * width)
                out[pl.ds(unit * UNIT * 8 + group * 64 + (tile - 8) * 8, 8 * width), :] = received[rows, :]

    begin(0)
    forward(1)
    settle(1)
    begin(1)
    go_on(0, 1)
    go_on(1, 1)
    go_on(0, 2)
    forward(2)
    go_on(1, 2)
    settle(2)
    exchange(2, 0, True, True)
    go_on(0, 3)
    exchange(2, 1, False, True)
    go_on(1, 3)
    go_on(2, 1)
    finish(0)
    finish(1)
    go_on(2, 2)
    take(0)
    go_on(2, 3)
    take(1)
    finish(2)

    for distance, copy, across in early:
        pl.when(sends(distance) & reads_early(distance))(copy.wait_send)
        pl.when(receives(distance) & reads_early(distance))(across.wait_send)
    for _, distance, first, count, copy, across in fetched:
        pl.when(sends(distance) & is_needed(first, count))(copy.wait_send)
        pl.when(receives(distance) & is_needed(first, count))(across.wait_send)
    to_partner.wait_send()
    for entry in messages:
        copy_of(*entry).wait_send()
    for phase, (tile, _) in enumerate(PHASES):
        if tile >= 8:
            for unit in range(UNITS):
                ship(phase, unit).wait_send()


def per_device(band_state, lower_rows, upper_rows, delays, counts):
    blocks = band_state.reshape(16, 8, 8, 128).transpose(0, 2, 1, 3).reshape(16, 64, 128)
    message_count = len(PHASES) * 2 * 4 * UNITS
    operands = (blocks, lower_rows, upper_rows, delays, counts)
    dma = pltpu.SemaphoreType.DMA
    out = pl.pallas_call(
        kernel,
        out_shape=jax.ShapeDtypeStruct((1024, 128), jnp.float32),
        in_specs=[pl.BlockSpec(memory_space=pltpu.HBM)] * 5,
        out_specs=pl.BlockSpec(memory_space=pltpu.VMEM),
        scratch_shapes=[
            pltpu.VMEM((2 * (GROUPS + 1), SPAN, 128), jnp.float32),
            pltpu.VMEM((ITERS, DMAX), jnp.int32),
            pltpu.VMEM((ITERS, DMAX), jnp.int32),
            pltpu.VMEM((ITERS, DMAX), jnp.int32),
            pltpu.SMEM((7,), jnp.int32),
            pltpu.VMEM((CHIPS, ROWS), jnp.int32),
            pltpu.SMEM((CHIPS, ROWS), jnp.int32),
            pltpu.VMEM((MESSAGE_ROWS[-1], 128), jnp.float32),
            pltpu.VMEM((MESSAGE_ROWS[-1], 128), jnp.float32),
            pltpu.VMEM((len(LATE), GROUPS, LATE_TILES * 8, 128), jnp.float32),
            pltpu.VMEM((RESULT_ROWS[-1], 128), jnp.float32),
            pltpu.VMEM((RESULT_ROWS[-1], 128), jnp.float32),
            pltpu.VMEM((UNIT * max(width for _, width in PHASES), 128), jnp.float32),
            dma,
            dma((4,)),
            dma((2,)),
            dma((4 * PARTS * len(FETCHES[0]),)),
            dma((4 * len(LATE),)),
            dma((message_count,)),
            dma((message_count,)),
            dma((2, len(PHASES) * UNITS)),
        ],
        compiler_params=pltpu.CompilerParams(collective_id=0, has_side_effects=True, vmem_limit_bytes=48 << 20),
    )(*(pltpu.with_memory_space_constraint(operand, pltpu.HBM) for operand in operands))
    return out.reshape(16, 8, 8, 128).transpose(0, 2, 1, 3).reshape(ROWS, 1024)


def solution(mesh):
    return jax.shard_map(
        per_device,
        mesh=mesh,
        in_specs=(P("freq", "tm"), P(), P(), P(), P()),
        out_specs=P("freq", "tm"),
        check_vma=False,
    )
```

```python
import jax
import jax.numpy as jnp
from jax import lax
from jax.experimental import pallas as pl
from jax.experimental.pallas import tpu as pltpu
from jax.sharding import PartitionSpec as P

DMAX = 2048
ITERS = 3
MESH = pl.DeviceIdType.MESH

CHIPS = 8
ROWS = 128
GROUPS = 32
TILES = 23
SPAN = TILES * 8
SET = (GROUPS + 1) * SPAN
HERE = 11
SKEW = 4
UNIT = 64
UNITS = ROWS // UNIT
FINISH_ORDER = [unit + side * UNITS // 2 for unit in range(UNITS // 2) for side in range(2)]
ZERO_ROW = GROUPS * SPAN
PHASES = ((10, 2), (8, 2), (4, 4))
PARTS = 1

FETCHES = (((-1, 4, 4), (1, 0, 4)), ((-1, 2, 2),), ((-1, 0, 2), (-2, 6, 2)))
LATE = tuple((phase, *piece) for phase in range(1, len(PHASES)) for piece in FETCHES[phase])
LATE_TILES = max(piece[3] for piece in LATE)

MESSAGE_ROWS = [sum(2 * 4 * ROWS * width for _, width in PHASES[:phase]) for phase in range(len(PHASES) + 1)]
RESULT_ROWS = [sum(ROWS * width for _, width in PHASES[:phase]) for phase in range(len(PHASES) + 1)]


def kernel(
    x, lower, upper, delays, counts, out,
    raw, lower_table, upper_table, delay_table, live, packed, picks, sent, landed, late, shipped, received, partial,
    local_sem, table_sem, own_sem, early_sem, late_sem, send_sem, recv_sem, ship_sem,
):
    freq = lax.axis_index("freq")
    tm = lax.axis_index("tm")
    tm_count = lax.axis_size("tm")
    z = lax.div(freq, 2)
    core = lax.rem(freq, 2)
    bits = [lax.rem(z, 2), lax.rem(lax.div(z, 2), 2), lax.div(z, 4)]
    partner = {"freq": freq + 1 - 2 * core}
    ring = ({"freq": lax.rem(freq + 2, 16)}, {"freq": lax.rem(freq + 14, 16)})
    flat = raw.reshape(2 * SET, 128)
    mine = pl.ds(core * 16, 16)

    def ahead(distance):
        return {"tm": lax.rem(tm + tm_count + distance, tm_count)}

    def tiles(first, count):
        return pl.ds((HERE + first) * 8, count * 8)

    own = pltpu.make_async_copy(x, raw.at[mine, tiles(0, 8), :], local_sem)
    own.start()
    tables = [
        pltpu.make_async_copy(source, target, table_sem.at[n])
        for n, (source, target) in enumerate(
            ((lower, lower_table), (upper, upper_table), (delays, delay_table), (counts, live))
        )
    ]
    for table in tables:
        table.start()

    barrier = pltpu.get_barrier_semaphore()
    peers = [partner, *ring, ahead(1), ahead(-1), ahead(2), ahead(-2)]
    for peer in peers:
        pl.semaphore_signal(barrier, inc=1, device_id=peer, device_id_type=MESH)
    pl.semaphore_wait(barrier, len(peers))

    own.wait()

    def remote(source, target, send, recv, device):
        return pltpu.make_async_remote_copy(
            src_ref=source, dst_ref=target, send_sem=send, recv_sem=recv,
            device_id=device, device_id_type=MESH,
        )

    def sends(distance):
        return tm < tm_count + distance if distance < 0 else tm >= 0

    def receives(distance):
        return tm >= -distance if distance < 0 else tm >= 0

    def first_chip(phase, tile):
        return (PHASES[phase][0] - tile) // 2 + 1

    size = 16 // PARTS
    shares = [pl.ds(core * 16 + part * size, size) for part in range(PARTS)]
    early = []
    for distance, first, count in FETCHES[0]:
        for share in shares:
            place = raw.at[share, tiles(distance * 8 + first, count), :]
            n = 4 * len(early)
            early.append((
                distance,
                remote(raw.at[share, tiles(first, count), :], place, early_sem.at[n], early_sem.at[n + 1], ahead(-distance)),
                remote(place, place, early_sem.at[n + 2], early_sem.at[n + 3], partner),
            ))
    early = [entry for part in range(PARTS) for entry in early[part::PARTS]]
    fetched = []
    for n, (phase, distance, first, count) in enumerate(LATE):
        place = late.at[n, mine, pl.ds(0, count * 8), :]
        fetched.append((
            phase, distance, distance * 8 + first, count,
            remote(raw.at[mine, tiles(first, count), :], place, late_sem.at[4 * n], late_sem.at[4 * n + 1], ahead(-distance)),
            remote(place, place, late_sem.at[4 * n + 2], late_sem.at[4 * n + 3], partner),
        ))
    to_partner = remote(
        raw.at[mine, tiles(0, 8), :], raw.at[mine, tiles(0, 8), :], own_sem.at[0], own_sem.at[1], partner
    )

    def reads_early(distance):
        return z >= first_chip(len(PHASES) - 1, 0) if distance < 0 else z >= 0

    for distance, copy, _ in early:
        pl.when(sends(distance) & reads_early(distance))(copy.start)
    def is_needed(first, count):
        return z >= first_chip(len(PHASES) - 1, first + count)

    for _, distance, first, count, copy, _ in fetched:
        pl.when(sends(distance) & is_needed(first, count))(copy.start)
    to_partner.start()

    def clear(base, first, count):
        def body(g, carry):
            raw[base + g, tiles(first, count), :] = jnp.zeros((count * 8, 128), jnp.float32)
            return carry
        lax.fori_loop(0, GROUPS, body, 0)

    raw[GROUPS, :, :] = jnp.zeros((SPAN, 128), jnp.float32)

    @pl.when(tm == 0)
    def _():
        clear(0, -10, 10)

    @pl.when(tm == 1)
    def _():
        clear(0, -10, 2)

    @pl.when(tm == tm_count - 1)
    def _():
        clear(GROUPS + 1, -HERE, HERE + 8)
        raw[2 * GROUPS + 1, :, :] = jnp.zeros((SPAN, 128), jnp.float32)

    for table in tables:
        table.wait()

    def entries(k, block):
        at = (pl.ds(k, 1), pl.ds(block, 128))
        row = jnp.where(bits[k] == 1, upper_table[at], lower_table[at])
        return row * 2048 + delay_table[at] * bits[k]

    def look_up(k, index):
        found = jnp.zeros((8, 128), jnp.int32)
        for block in range(DMAX // 128):
            table = jnp.broadcast_to(entries(k, block * 128), (8, 128))
            here = jnp.take_along_axis(table, index & 127, axis=1)
            found = jnp.where(index >> 7 == block, here, found)
        return found

    def is_live(k, index):
        bands = 4 >> k
        width = DMAX // bands
        first = 8 - (8 >> k)
        count = jnp.full((8, 128), live[first], jnp.int32)
        for band in range(1, bands):
            count = jnp.where(index // width == band, live[first + band], count)
        return (index & (width - 1)) < count

    for offset in range(CHIPS):
        block = lax.rem(z + offset, CHIPS) * 256 + core * ROWS
        packed[pl.ds(offset, 1), :] = entries(2, pl.multiple_of(block, 128))
    top = packed[...]
    middle = look_up(1, top >> 11)
    bottom = look_up(0, middle >> 11)
    delay = (top & 2047) + (middle & 2047) + (bottom & 2047)
    row = (bottom >> 11) & 255
    start = (row >> 3) * SPAN + (row & 7) + (HERE - (delay >> 7)) * 8
    start = jnp.where(is_live(1, top >> 11) & is_live(0, middle >> 11), start, ZERO_ROW + HERE * 8)
    packed[...] = start * 128 + (delay & 127)
    to_scalar = pltpu.make_async_copy(packed, picks, table_sem.at[0])
    to_scalar.start()
    to_scalar.wait()

    for distance, copy, across in early:
        @pl.when(receives(distance) & reads_early(distance))
        def _(copy=copy, across=across):
            copy.wait_recv()
            across.start()
    to_partner.wait_recv()
    for distance, _, across in early:
        pl.when(receives(distance) & reads_early(distance))(across.wait_recv)

    @pl.when(tm == tm_count - 1)
    def _():
        def body(g, carry):
            raw[GROUPS + 1 + g, tiles(8, SKEW), :] = raw[g, tiles(8, SKEW), :]
            return carry
        lax.fori_loop(0, GROUPS, body, 0)

    def when_first_read(phase, distance, first, count):
        here = receives(distance) & (z >= first_chip(phase, first + count))
        return here & (z < first_chip(phase - 1, first + count)) if phase > 1 else here

    def forward(phase):
        for when, distance, first, count, copy, across in fetched:
            if when <= phase:
                @pl.when(when_first_read(phase, distance, first, count))
                def _(copy=copy, across=across):
                    copy.wait_recv()
                    across.start()

    def settle(phase):
        for n, (when, distance, first, count, _, across) in enumerate(fetched):
            if when <= phase:
                @pl.when(when_first_read(phase, distance, first, count))
                def _(n=n, first=first, count=count, across=across):
                    across.wait_recv()

                    def body(g, carry):
                        raw[g, tiles(first, count), :] = late[n, g, pl.ds(0, count * 8), :]
                        return carry
                    lax.fori_loop(0, GROUPS, body, 0)

    wrapped = jnp.where(tm == tm_count - 1, SET, 0)

    def contribution(phase, offset, row):
        tile, width = PHASES[phase]
        entry = picks[offset, row]
        start = (entry >> 7) + tile * 8
        if tile >= 8:
            start = start + wrapped
        shift = entry & 127
        same = flat[pl.ds(start, width, stride=8), :]
        before = flat[pl.ds(start - 8, width, stride=8), :]
        lanes = lax.broadcasted_iota(jnp.int32, (width, 128), 1)
        return pltpu.roll(jnp.where(lanes < 128 - shift, same, before), shift, 1)

    def first_row(phase, direction, step, unit):
        return MESSAGE_ROWS[phase] + ((direction * 4 + step) * UNITS + unit) * UNIT * PHASES[phase][1]

    def copy_of(phase, direction, step, unit):
        rows = pl.ds(first_row(phase, direction, step, unit), UNIT * PHASES[phase][1])
        n = ((phase * 2 + direction) * 4 + step) * UNITS + unit
        return remote(sent.at[rows, :], landed.at[rows, :], send_sem.at[n], recv_sem.at[n], ring[direction])

    def is_long(direction, unit):
        return (unit < UNITS // 2) == (direction == 0)

    messages = []

    def add_and_send(phase, direction, step, unit, fresh):
        width = PHASES[phase][1]
        offset = 4 - step if direction == 0 else 4 + step
        target = first_row(phase, direction, step, unit)
        source = first_row(phase, direction, step - 1, unit)
        if not fresh:
            copy_of(phase, direction, step - 1, unit).wait_recv()

        for row in range(UNIT):
            value = contribution(phase, offset, unit * UNIT + row)
            if not fresh:
                value = value + landed[pl.ds(source + row * width, width), :]
            sent[pl.ds(target + row * width, width), :] = value
        copy_of(phase, direction, step, unit).start()
        messages.append((phase, direction, step, unit))

    def exchange(phase, step, long, fresh):
        for unit in range(UNITS):
            for direction in range(2):
                if is_long(direction, unit) == long:
                    add_and_send(phase, direction, step, unit, fresh)

    def begin(phase):
        exchange(phase, 0, True, True)
        exchange(phase, 1, False, True)

    def go_on(phase, step):
        if step > 1:
            exchange(phase, step, False, False)
        exchange(phase, step, True, False)

    def ship(phase, unit):
        width = PHASES[phase][1]
        rows = pl.ds(RESULT_ROWS[phase] + unit * UNIT * width, UNIT * width)
        n = phase * UNITS + unit
        return remote(shipped.at[rows, :], received.at[rows, :], ship_sem.at[0, n], ship_sem.at[1, n], ahead(1))

    def finish(phase):
        tile, width = PHASES[phase]
        for unit in FINISH_ORDER:
            sources = [first_row(phase, direction, 3, unit) for direction in range(2)]
            last = 0 if is_long(0, unit) else 1
            copy_of(phase, 1 - last, 3, unit).wait_recv()
            for row in range(UNIT):
                value = contribution(phase, 0, unit * UNIT + row)
                value = value + landed[pl.ds(sources[1 - last] + row * width, width), :]
                alive = freq * ROWS + unit * UNIT + row < live[6]
                partial[pl.ds(row * width, width), :] = jnp.where(alive, value, jnp.zeros_like(value))
            copy_of(phase, last, 3, unit).wait_recv()
            for row in range(UNIT):
                alive = freq * ROWS + unit * UNIT + row < live[6]
                value = landed[pl.ds(sources[last] + row * width, width), :]
                value = partial[pl.ds(row * width, width), :] + jnp.where(alive, value, jnp.zeros_like(value))
                if tile >= 8:
                    at = RESULT_ROWS[phase] + unit * UNIT * width + (row // 8) * width * 8 + row % 8
                    shipped[pl.ds(at, width, stride=8), :] = value
                else:
                    out[pl.ds((unit * UNIT + row - row % 8) * 8 + tile * 8 + row % 8, width, stride=8), :] = value
            if tile >= 8:
                ship(phase, unit).start()

    def take(phase):
        tile, width = PHASES[phase]
        for unit in range(UNITS):
            ship(phase, unit).wait_recv()
            for group in range(UNIT // 8):
                rows = pl.ds(RESULT_ROWS[phase] + (unit * UNIT + group * 8) * width, 8 * width)
                out[pl.ds(unit * UNIT * 8 + group * 64 + (tile - 8) * 8, 8 * width), :] = received[rows, :]

    begin(0)
    forward(1)
    settle(1)
    exchange(1, 0, True, True)
    go_on(0, 1)
    exchange(1, 1, False, True)
    go_on(1, 1)
    go_on(0, 2)
    forward(2)
    go_on(1, 2)
    settle(2)
    exchange(2, 0, True, True)
    go_on(0, 3)
    exchange(2, 1, False, True)
    go_on(1, 3)
    go_on(2, 1)
    finish(0)
    finish(1)
    go_on(2, 2)
    take(0)
    go_on(2, 3)
    take(1)
    finish(2)

    for distance, copy, across in early:
        pl.when(sends(distance) & reads_early(distance))(copy.wait_send)
        pl.when(receives(distance) & reads_early(distance))(across.wait_send)
    for _, distance, first, count, copy, across in fetched:
        pl.when(sends(distance) & is_needed(first, count))(copy.wait_send)
        pl.when(receives(distance) & is_needed(first, count))(across.wait_send)
    to_partner.wait_send()
    for entry in messages:
        copy_of(*entry).wait_send()
    for phase, (tile, _) in enumerate(PHASES):
        if tile >= 8:
            for unit in range(UNITS):
                ship(phase, unit).wait_send()


def per_device(band_state, lower_rows, upper_rows, delays, counts):
    blocks = band_state.reshape(16, 8, 8, 128).transpose(0, 2, 1, 3).reshape(16, 64, 128)
    message_count = len(PHASES) * 2 * 4 * UNITS
    operands = (blocks, lower_rows, upper_rows, delays, counts)
    dma = pltpu.SemaphoreType.DMA
    out = pl.pallas_call(
        kernel,
        out_shape=jax.ShapeDtypeStruct((1024, 128), jnp.float32),
        in_specs=[pl.BlockSpec(memory_space=pltpu.HBM)] * 5,
        out_specs=pl.BlockSpec(memory_space=pltpu.VMEM),
        scratch_shapes=[
            pltpu.VMEM((2 * (GROUPS + 1), SPAN, 128), jnp.float32),
            pltpu.VMEM((ITERS, DMAX), jnp.int32),
            pltpu.VMEM((ITERS, DMAX), jnp.int32),
            pltpu.VMEM((ITERS, DMAX), jnp.int32),
            pltpu.SMEM((7,), jnp.int32),
            pltpu.VMEM((CHIPS, ROWS), jnp.int32),
            pltpu.SMEM((CHIPS, ROWS), jnp.int32),
            pltpu.VMEM((MESSAGE_ROWS[-1], 128), jnp.float32),
            pltpu.VMEM((MESSAGE_ROWS[-1], 128), jnp.float32),
            pltpu.VMEM((len(LATE), GROUPS, LATE_TILES * 8, 128), jnp.float32),
            pltpu.VMEM((RESULT_ROWS[-1], 128), jnp.float32),
            pltpu.VMEM((RESULT_ROWS[-1], 128), jnp.float32),
            pltpu.VMEM((UNIT * max(width for _, width in PHASES), 128), jnp.float32),
            dma,
            dma((4,)),
            dma((2,)),
            dma((4 * PARTS * len(FETCHES[0]),)),
            dma((4 * len(LATE),)),
            dma((message_count,)),
            dma((message_count,)),
            dma((2, len(PHASES) * UNITS)),
        ],
        compiler_params=pltpu.CompilerParams(collective_id=0, has_side_effects=True, vmem_limit_bytes=48 << 20),
    )(*(pltpu.with_memory_space_constraint(operand, pltpu.HBM) for operand in operands))
    return out.reshape(16, 8, 8, 128).transpose(0, 2, 1, 3).reshape(ROWS, 1024)


def solution(mesh):
    return jax.shard_map(
        per_device,
        mesh=mesh,
        in_specs=(P("freq", "tm"), P(), P(), P(), P()),
        out_specs=P("freq", "tm"),
        check_vma=False,
    )
```

```python
import jax
import jax.numpy as jnp
from jax import lax
from jax.experimental import pallas as pl
from jax.experimental.pallas import tpu as pltpu
from jax.sharding import PartitionSpec as P

DMAX = 2048
ITERS = 3
MESH = pl.DeviceIdType.MESH

CHIPS = 8
ROWS = 128
GROUPS = 32
TILES = 23
SPAN = TILES * 8
SET = (GROUPS + 1) * SPAN
HERE = 11
SKEW = 4
UNIT = 64
UNITS = ROWS // UNIT
FINISH_ORDER = [unit + side * UNITS // 2 for unit in range(UNITS // 2) for side in range(2)]
ZERO_ROW = GROUPS * SPAN
PHASES = ((10, 2), (8, 2), (4, 4))
PARTS = 1

FETCHES = (((-1, 4, 4), (1, 0, 4)), ((-1, 2, 2),), ((-1, 0, 2), (-2, 6, 2)))
LATE = tuple((phase, *piece) for phase in range(1, len(PHASES)) for piece in FETCHES[phase])
LATE_TILES = max(piece[3] for piece in LATE)

MESSAGE_ROWS = [sum(2 * 4 * ROWS * width for _, width in PHASES[:phase]) for phase in range(len(PHASES) + 1)]
RESULT_ROWS = [sum(ROWS * width for _, width in PHASES[:phase]) for phase in range(len(PHASES) + 1)]


def kernel(
    x, lower, upper, delays, counts, out,
    raw, lower_table, upper_table, delay_table, live, packed, picks, sent, landed, late, shipped, received, partial,
    local_sem, table_sem, own_sem, early_sem, late_sem, send_sem, recv_sem, ship_sem,
):
    freq = lax.axis_index("freq")
    tm = lax.axis_index("tm")
    tm_count = lax.axis_size("tm")
    z = lax.div(freq, 2)
    core = lax.rem(freq, 2)
    bits = [lax.rem(z, 2), lax.rem(lax.div(z, 2), 2), lax.div(z, 4)]
    partner = {"freq": freq + 1 - 2 * core}
    ring = ({"freq": lax.rem(freq + 2, 16)}, {"freq": lax.rem(freq + 14, 16)})
    flat = raw.reshape(2 * SET, 128)
    mine = pl.ds(core * 16, 16)

    def ahead(distance):
        return {"tm": lax.rem(tm + tm_count + distance, tm_count)}

    def tiles(first, count):
        return pl.ds((HERE + first) * 8, count * 8)

    own = pltpu.make_async_copy(x, raw.at[mine, tiles(0, 8), :], local_sem)
    own.start()
    tables = [
        pltpu.make_async_copy(source, target, table_sem.at[n])
        for n, (source, target) in enumerate(
            ((lower, lower_table), (upper, upper_table), (delays, delay_table), (counts, live))
        )
    ]
    for table in tables:
        table.start()

    barrier = pltpu.get_barrier_semaphore()
    peers = [partner, *ring, ahead(1), ahead(-1), ahead(2), ahead(-2)]
    for peer in peers:
        pl.semaphore_signal(barrier, inc=1, device_id=peer, device_id_type=MESH)
    pl.semaphore_wait(barrier, len(peers))

    own.wait()

    def remote(source, target, send, recv, device):
        return pltpu.make_async_remote_copy(
            src_ref=source, dst_ref=target, send_sem=send, recv_sem=recv,
            device_id=device, device_id_type=MESH,
        )

    def sends(distance):
        return tm < tm_count + distance if distance < 0 else tm >= 0

    def receives(distance):
        return tm >= -distance if distance < 0 else tm >= 0

    def first_chip(phase, tile):
        return (PHASES[phase][0] - tile) // 2 + 1

    size = 16 // PARTS
    shares = [pl.ds(core * 16 + part * size, size) for part in range(PARTS)]
    early = []
    for distance, first, count in FETCHES[0]:
        for share in shares:
            place = raw.at[share, tiles(distance * 8 + first, count), :]
            n = 4 * len(early)
            early.append((
                distance,
                remote(raw.at[share, tiles(first, count), :], place, early_sem.at[n], early_sem.at[n + 1], ahead(-distance)),
                remote(place, place, early_sem.at[n + 2], early_sem.at[n + 3], partner),
            ))
    early = [entry for part in range(PARTS) for entry in early[part::PARTS]]
    fetched = []
    for n, (phase, distance, first, count) in enumerate(LATE):
        place = late.at[n, mine, pl.ds(0, count * 8), :]
        fetched.append((
            phase, distance, distance * 8 + first, count,
            remote(raw.at[mine, tiles(first, count), :], place, late_sem.at[4 * n], late_sem.at[4 * n + 1], ahead(-distance)),
            remote(place, place, late_sem.at[4 * n + 2], late_sem.at[4 * n + 3], partner),
        ))
    to_partner = remote(
        raw.at[mine, tiles(0, 8), :], raw.at[mine, tiles(0, 8), :], own_sem.at[0], own_sem.at[1], partner
    )

    def reads_early(distance):
        return z >= first_chip(len(PHASES) - 1, 0) if distance < 0 else z >= 0

    for distance, copy, _ in early:
        pl.when(sends(distance) & reads_early(distance))(copy.start)
    def is_needed(first, count):
        return z >= first_chip(len(PHASES) - 1, first + count)

    def request(phase):
        for when, distance, first, count, copy, _ in fetched:
            if when == phase:
                pl.when(sends(distance) & is_needed(first, count))(copy.start)

    request(1)
    to_partner.start()

    def clear(base, first, count):
        def body(g, carry):
            raw[base + g, tiles(first, count), :] = jnp.zeros((count * 8, 128), jnp.float32)
            return carry
        lax.fori_loop(0, GROUPS, body, 0)

    raw[GROUPS, :, :] = jnp.zeros((SPAN, 128), jnp.float32)

    @pl.when(tm == 0)
    def _():
        clear(0, -10, 10)

    @pl.when(tm == 1)
    def _():
        clear(0, -10, 2)

    @pl.when(tm == tm_count - 1)
    def _():
        clear(GROUPS + 1, -HERE, HERE + 8)
        raw[2 * GROUPS + 1, :, :] = jnp.zeros((SPAN, 128), jnp.float32)

    for table in tables:
        table.wait()

    def entries(k, block):
        at = (pl.ds(k, 1), pl.ds(block, 128))
        row = jnp.where(bits[k] == 1, upper_table[at], lower_table[at])
        return row * 2048 + delay_table[at] * bits[k]

    def look_up(k, index):
        found = jnp.zeros((8, 128), jnp.int32)
        for block in range(DMAX // 128):
            table = jnp.broadcast_to(entries(k, block * 128), (8, 128))
            here = jnp.take_along_axis(table, index & 127, axis=1)
            found = jnp.where(index >> 7 == block, here, found)
        return found

    def is_live(k, index):
        bands = 4 >> k
        width = DMAX // bands
        first = 8 - (8 >> k)
        count = jnp.full((8, 128), live[first], jnp.int32)
        for band in range(1, bands):
            count = jnp.where(index // width == band, live[first + band], count)
        return (index & (width - 1)) < count

    for offset in range(CHIPS):
        block = lax.rem(z + offset, CHIPS) * 256 + core * ROWS
        packed[pl.ds(offset, 1), :] = entries(2, pl.multiple_of(block, 128))
    top = packed[...]
    middle = look_up(1, top >> 11)
    bottom = look_up(0, middle >> 11)
    delay = (top & 2047) + (middle & 2047) + (bottom & 2047)
    row = (bottom >> 11) & 255
    start = (row >> 3) * SPAN + (row & 7) + (HERE - (delay >> 7)) * 8
    start = jnp.where(is_live(1, top >> 11) & is_live(0, middle >> 11), start, ZERO_ROW + HERE * 8)
    packed[...] = start * 128 + (delay & 127)
    to_scalar = pltpu.make_async_copy(packed, picks, table_sem.at[0])
    to_scalar.start()
    to_scalar.wait()

    for distance, copy, across in early:
        @pl.when(receives(distance) & reads_early(distance))
        def _(copy=copy, across=across):
            copy.wait_recv()
            across.start()
    to_partner.wait_recv()
    for distance, _, across in early:
        pl.when(receives(distance) & reads_early(distance))(across.wait_recv)

    @pl.when(tm == tm_count - 1)
    def _():
        def body(g, carry):
            raw[GROUPS + 1 + g, tiles(8, SKEW), :] = raw[g, tiles(8, SKEW), :]
            return carry
        lax.fori_loop(0, GROUPS, body, 0)

    def when_first_read(phase, distance, first, count):
        here = receives(distance) & (z >= first_chip(phase, first + count))
        return here & (z < first_chip(phase - 1, first + count)) if phase > 1 else here

    def forward(phase):
        for when, distance, first, count, copy, across in fetched:
            if when <= phase:
                @pl.when(when_first_read(phase, distance, first, count))
                def _(copy=copy, across=across):
                    copy.wait_recv()
                    across.start()

    def settle(phase):
        for n, (when, distance, first, count, _, across) in enumerate(fetched):
            if when <= phase:
                @pl.when(when_first_read(phase, distance, first, count))
                def _(n=n, first=first, count=count, across=across):
                    across.wait_recv()

                    def body(g, carry):
                        raw[g, tiles(first, count), :] = late[n, g, pl.ds(0, count * 8), :]
                        return carry
                    lax.fori_loop(0, GROUPS, body, 0)

    wrapped = jnp.where(tm == tm_count - 1, SET, 0)

    def contribution(phase, offset, row):
        tile, width = PHASES[phase]
        entry = picks[offset, row]
        start = (entry >> 7) + tile * 8
        if tile >= 8:
            start = start + wrapped
        shift = entry & 127
        same = flat[pl.ds(start, width, stride=8), :]
        before = flat[pl.ds(start - 8, width, stride=8), :]
        lanes = lax.broadcasted_iota(jnp.int32, (width, 128), 1)
        return pltpu.roll(jnp.where(lanes < 128 - shift, same, before), shift, 1)

    def first_row(phase, direction, step, unit):
        return MESSAGE_ROWS[phase] + ((direction * 4 + step) * UNITS + unit) * UNIT * PHASES[phase][1]

    def copy_of(phase, direction, step, unit):
        rows = pl.ds(first_row(phase, direction, step, unit), UNIT * PHASES[phase][1])
        n = ((phase * 2 + direction) * 4 + step) * UNITS + unit
        return remote(sent.at[rows, :], landed.at[rows, :], send_sem.at[n], recv_sem.at[n], ring[direction])

    def is_long(direction, unit):
        return (unit < UNITS // 2) == (direction == 0)

    messages = []

    def add_and_send(phase, direction, step, unit, fresh):
        width = PHASES[phase][1]
        offset = 4 - step if direction == 0 else 4 + step
        target = first_row(phase, direction, step, unit)
        source = first_row(phase, direction, step - 1, unit)
        if not fresh:
            copy_of(phase, direction, step - 1, unit).wait_recv()

        for row in range(UNIT):
            value = contribution(phase, offset, unit * UNIT + row)
            if not fresh:
                value = value + landed[pl.ds(source + row * width, width), :]
            sent[pl.ds(target + row * width, width), :] = value
        copy_of(phase, direction, step, unit).start()
        messages.append((phase, direction, step, unit))

    def exchange(phase, step, long, fresh):
        for unit in range(UNITS):
            for direction in range(2):
                if is_long(direction, unit) == long:
                    add_and_send(phase, direction, step, unit, fresh)

    def begin(phase):
        exchange(phase, 0, True, True)
        exchange(phase, 1, False, True)

    def go_on(phase, step):
        if step > 1:
            exchange(phase, step, False, False)
        exchange(phase, step, True, False)

    def ship(phase, unit):
        width = PHASES[phase][1]
        rows = pl.ds(RESULT_ROWS[phase] + unit * UNIT * width, UNIT * width)
        n = phase * UNITS + unit
        return remote(shipped.at[rows, :], received.at[rows, :], ship_sem.at[0, n], ship_sem.at[1, n], ahead(1))

    def finish(phase):
        tile, width = PHASES[phase]
        for unit in FINISH_ORDER:
            sources = [first_row(phase, direction, 3, unit) for direction in range(2)]
            last = 0 if is_long(0, unit) else 1
            copy_of(phase, 1 - last, 3, unit).wait_recv()
            for row in range(UNIT):
                value = contribution(phase, 0, unit * UNIT + row)
                value = value + landed[pl.ds(sources[1 - last] + row * width, width), :]
                alive = freq * ROWS + unit * UNIT + row < live[6]
                partial[pl.ds(row * width, width), :] = jnp.where(alive, value, jnp.zeros_like(value))
            copy_of(phase, last, 3, unit).wait_recv()
            for row in range(UNIT):
                alive = freq * ROWS + unit * UNIT + row < live[6]
                value = landed[pl.ds(sources[last] + row * width, width), :]
                value = partial[pl.ds(row * width, width), :] + jnp.where(alive, value, jnp.zeros_like(value))
                if tile >= 8:
                    at = RESULT_ROWS[phase] + unit * UNIT * width + (row // 8) * width * 8 + row % 8
                    shipped[pl.ds(at, width, stride=8), :] = value
                else:
                    out[pl.ds((unit * UNIT + row - row % 8) * 8 + tile * 8 + row % 8, width, stride=8), :] = value
            if tile >= 8:
                ship(phase, unit).start()

    def take(phase):
        tile, width = PHASES[phase]
        for unit in range(UNITS):
            ship(phase, unit).wait_recv()
            for group in range(UNIT // 8):
                rows = pl.ds(RESULT_ROWS[phase] + (unit * UNIT + group * 8) * width, 8 * width)
                out[pl.ds(unit * UNIT * 8 + group * 64 + (tile - 8) * 8, 8 * width), :] = received[rows, :]

    begin(0)
    forward(1)
    settle(1)
    begin(1)
    request(2)
    go_on(0, 1)
    go_on(1, 1)
    go_on(0, 2)
    forward(2)
    go_on(1, 2)
    settle(2)
    exchange(2, 0, True, True)
    go_on(0, 3)
    exchange(2, 1, False, True)
    go_on(1, 3)
    go_on(2, 1)
    finish(0)
    finish(1)
    go_on(2, 2)
    take(0)
    go_on(2, 3)
    take(1)
    finish(2)

    for distance, copy, across in early:
        pl.when(sends(distance) & reads_early(distance))(copy.wait_send)
        pl.when(receives(distance) & reads_early(distance))(across.wait_send)
    for _, distance, first, count, copy, across in fetched:
        pl.when(sends(distance) & is_needed(first, count))(copy.wait_send)
        pl.when(receives(distance) & is_needed(first, count))(across.wait_send)
    to_partner.wait_send()
    for entry in messages:
        copy_of(*entry).wait_send()
    for phase, (tile, _) in enumerate(PHASES):
        if tile >= 8:
            for unit in range(UNITS):
                ship(phase, unit).wait_send()


def per_device(band_state, lower_rows, upper_rows, delays, counts):
    blocks = band_state.reshape(16, 8, 8, 128).transpose(0, 2, 1, 3).reshape(16, 64, 128)
    message_count = len(PHASES) * 2 * 4 * UNITS
    operands = (blocks, lower_rows, upper_rows, delays, counts)
    dma = pltpu.SemaphoreType.DMA
    out = pl.pallas_call(
        kernel,
        out_shape=jax.ShapeDtypeStruct((1024, 128), jnp.float32),
        in_specs=[pl.BlockSpec(memory_space=pltpu.HBM)] * 5,
        out_specs=pl.BlockSpec(memory_space=pltpu.VMEM),
        scratch_shapes=[
            pltpu.VMEM((2 * (GROUPS + 1), SPAN, 128), jnp.float32),
            pltpu.VMEM((ITERS, DMAX), jnp.int32),
            pltpu.VMEM((ITERS, DMAX), jnp.int32),
            pltpu.VMEM((ITERS, DMAX), jnp.int32),
            pltpu.SMEM((7,), jnp.int32),
            pltpu.VMEM((CHIPS, ROWS), jnp.int32),
            pltpu.SMEM((CHIPS, ROWS), jnp.int32),
            pltpu.VMEM((MESSAGE_ROWS[-1], 128), jnp.float32),
            pltpu.VMEM((MESSAGE_ROWS[-1], 128), jnp.float32),
            pltpu.VMEM((len(LATE), GROUPS, LATE_TILES * 8, 128), jnp.float32),
            pltpu.VMEM((RESULT_ROWS[-1], 128), jnp.float32),
            pltpu.VMEM((RESULT_ROWS[-1], 128), jnp.float32),
            pltpu.VMEM((UNIT * max(width for _, width in PHASES), 128), jnp.float32),
            dma,
            dma((4,)),
            dma((2,)),
            dma((4 * PARTS * len(FETCHES[0]),)),
            dma((4 * len(LATE),)),
            dma((message_count,)),
            dma((message_count,)),
            dma((2, len(PHASES) * UNITS)),
        ],
        compiler_params=pltpu.CompilerParams(collective_id=0, has_side_effects=True, vmem_limit_bytes=48 << 20),
    )(*(pltpu.with_memory_space_constraint(operand, pltpu.HBM) for operand in operands))
    return out.reshape(16, 8, 8, 128).transpose(0, 2, 1, 3).reshape(ROWS, 1024)


def solution(mesh):
    return jax.shard_map(
        per_device,
        mesh=mesh,
        in_specs=(P("freq", "tm"), P(), P(), P(), P()),
        out_specs=P("freq", "tm"),
        check_vma=False,
    )
```
